32 devices in a mesh: dp: 4 (over y, x), expert: 8 (over z, core).
Axes of the slice: x: 2, y: 2, z: 4, core: 2. Of those that a mesh axis runs over, the one named last changes fastest.
Arguments:
- tokens: bfloat16 [4096, 2048], P(('dp', 'expert')), may hold values from -6 to 6
- expert_ids: int32 [4096, 2], P(('dp', 'expert')), may hold values from 0 to 7, all different within a row; in each aligned block of 128 rows (0 to 127, 128 to 255, ...) at most 48 rows name the same one
- route_weights: float32 [4096, 2], P(('dp', 'expert')), may hold values from 0.1 to 1
- w_gate: bfloat16 [8, 2048, 384], P('expert', 'dp'), may hold values from -0.125 to 0.125
- w_up: bfloat16 [8, 2048, 384], P('expert', 'dp'), may hold values from -0.125 to 0.125
- w_down: bfloat16 [8, 2048, 384], P('expert', 'dp'), may hold values from -0.3125 to 0.3125
- grad_out: bfloat16 [4096, 2048], P(('dp', 'expert')), may hold values from -6 to 6
Outputs:
- layer_out: bfloat16 [4096, 2048], P(('dp', 'expert'))
- token_grad: bfloat16 [4096, 2048], P(('dp', 'expert'))
- route_grad: float32 [4096, 2], P(('dp', 'expert'))
- gate_grad: bfloat16 [8, 2048, 384], P('expert', 'dp')
- up_grad: bfloat16 [8, 2048, 384], P('expert', 'dp')
- down_grad: bfloat16 [8, 2048, 384], P('expert', 'dp')
The draws below stay inside these ranges and needn't reach their ends.
Inputs may be any that keep to these rules, and one draw needn't show every extreme that they name: `expert_ids`: each token names 2 different experts. Among the tokens of one device (aligned blocks of 128 tokens) no expert is named more than 48 times, and in some blocks one is named exactly 48 times.
All inputs are finite; a program needn't handle non-finite values.
Results may differ from the reference program's by a relative error of at most 0.0065.
Values may be sent and summed in bfloat16 or wider, within the bound.
A program may use at most 64 MiB of HBM per device.

```python
import math
import jax
import jax.numpy as jnp
import numpy as np
from jax import lax

D = 2048
FF = 384
TOP = 2
TOK_DEV = 128
EXPERTS = 8
TOKENS = 4096
CAP = 48
N_DP = 4
N_EXPERT = 8


def block_levels(stream_key, shape, cuts, low, high):
    level = 1.0
    for dim, blocks in cuts:
        steps = jax.random.uniform(jax.random.fold_in(jax.random.fold_in(stream_key, 6), dim), (blocks,), jnp.float32, low / len(cuts), high / len(cuts))
        level = level * jnp.repeat(jnp.exp(steps), shape[dim] // blocks).reshape((-1,) + (1,) * (len(shape) - 1 - dim))
    return level


def shared_out(key, own, number, rows, amount, top, limit, lean):
    sequence = jax.random.permutation(key, amount)
    crowded, common = load_shares(amount, rows * top, limit, lean, True), load_shares(amount, rows * top, limit, lean, False)
    places = jnp.arange(amount)

    def named(lengths, turn):
        used = int((lengths > 0).sum())
        fixed = max(1, used // 4)
        moved = fixed + (places - fixed + turn * (used - fixed)) % max(1, amount - fixed)
        return jnp.zeros((amount,), jnp.int32).at[sequence[jnp.where(places < fixed, places, moved)]].set(jnp.asarray(lengths, jnp.int32))

    lengths = jnp.where(number % 4 == 0, named(crowded, number // 4), named(common, number - number // 4 - 1))
    mixed = jax.random.permutation(jax.random.fold_in(own, 3), amount)
    giver, sink = mixed[0:amount // 2 * 2:2], mixed[1:amount // 2 * 2:2]
    margin = jnp.minimum(lengths[giver] - 1, limit - lengths[sink]) // 2
    margin = jnp.where((giver == sequence[0]) | (sink == sequence[0]) | (lengths[sink] == 0), 0, jnp.maximum(margin, 0))
    moved = jax.random.randint(jax.random.fold_in(own, 4), (amount // 2,), 0, 1 << 20) % (margin + 1)
    lengths = lengths.at[giver].add(-moved).at[sink].add(moved)
    labels = jnp.searchsorted(jnp.cumsum(lengths), jnp.arange(rows * top), side="right").astype(jnp.int32)
    listing = labels.reshape(top, rows).T
    listing = listing[jax.random.permutation(jax.random.fold_in(own, 1), rows)]
    turn = jax.random.randint(jax.random.fold_in(own, 2), (rows, 1), 0, top)
    return jnp.take_along_axis(listing, (jnp.arange(top)[None, :] + turn) % top, axis=1)


def load_shares(amount, total, reach, slope, full):
    loads = [(1 << 20) // math.isqrt(grade ** slope) + 1 for grade in range(1, amount + 1)]
    largest = reach if full else min(reach, max(-(-total // amount), total * loads[0] // sum(loads)))
    least = 1 if total - largest >= amount - 1 else 0
    counts, rest = [largest] + [least] * (amount - 1), total - largest - least * (amount - 1)
    while rest > 0:
        candidates = [i for i in range(1, amount) if counts[i] < largest] or [i for i in range(1, amount) if counts[i] < reach]
        pool, left = sum([loads[i] for i in candidates]), rest
        for i in candidates:
            addition = min(reach - counts[i], max(1, left * loads[i] // pool), rest)
            counts[i] = counts[i] + addition
            rest = rest - addition
    return np.array(counts)


def scatter_about(own_key, extent, width, most, shards=(), kind=jnp.bfloat16):
    drawn = width * jax.random.normal(own_key, extent, jnp.float32)
    if shards:
        drawn = drawn * block_levels(own_key, extent, shards, -0.22, 0.18)
    return jnp.clip(drawn, -most, most).astype(kind)


def setup_inputs(seed: int = 0) -> dict:
    splits = jax.random.split(jax.random.key(seed), 8)
    tokens = scatter_about(splits[0], (TOKENS, D), 1.0, 6.0, ((0, 32),))
    expert_ids_keys = jax.random.split(jax.random.fold_in(splits[1], 1), TOKENS // TOK_DEV)
    expert_ids_turns = jax.random.permutation(jax.random.fold_in(splits[1], 3), TOKENS // TOK_DEV)
    expert_ids = jax.vmap(lambda own, number: shared_out(jax.random.fold_in(splits[1], 2), own, number, TOK_DEV, EXPERTS, TOP, CAP, 2))(expert_ids_keys, expert_ids_turns).reshape((TOKENS, TOP))
    route_weights = jnp.clip(jnp.exp(math.log(1.0) - 2.3025851 * jax.random.uniform(splits[2], (TOKENS, TOP), jnp.float32) ** block_levels(splits[2], (TOKENS, TOP), ((0, 32),), -0.2, 0.2)), 0.1, 1.0)
    w_gate = scatter_about(splits[3], (EXPERTS, D, FF), D ** -0.5, 0.125, ((0, 8), (1, 4)))
    w_up = scatter_about(splits[4], (EXPERTS, D, FF), D ** -0.5, 0.125, ((0, 8), (1, 4)))
    w_down = scatter_about(splits[5], (EXPERTS, D, FF), FF ** -0.5, 0.3125, ((0, 8), (1, 4)))
    grad_out = scatter_about(splits[6], (TOKENS, D), 1.0, 6.0, ((0, 32),))
    return {"tokens": tokens, "expert_ids": expert_ids, "route_weights": route_weights, "w_gate": w_gate, "w_up": w_up, "w_down": w_down, "grad_out": grad_out}


def reference(tokens, expert_ids, route_weights, w_gate, w_up, w_down, grad_out):
    slots = TOKENS * TOP
    most_rows = N_DP * N_EXPERT * CAP
    flat_ids = expert_ids.reshape(-1)
    flat_weights = route_weights.reshape(-1)

    def one_expert(carry, expert):
        out_acc, grad_acc, route_acc = carry
        picked = jnp.nonzero(flat_ids == expert, size=most_rows, fill_value=slots)[0].astype(jnp.int32)
        valid = picked < slots
        slot = jnp.minimum(picked, slots - 1).astype(jnp.int32)
        token = (slot // TOP).astype(jnp.int32)
        live = valid.astype(jnp.float32)
        rows = jnp.where(valid[:, None], tokens[token], jnp.zeros((), jnp.bfloat16))
        weight = flat_weights[slot] * live
        cotan = grad_out[token].astype(jnp.float32)
        gate_w = w_gate[expert]
        up_w = w_up[expert]
        down_w = w_down[expert]
        gate = jnp.dot(rows, gate_w, preferred_element_type=jnp.float32)
        up = jnp.dot(rows, up_w, preferred_element_type=jnp.float32)
        sig = jax.nn.sigmoid(gate)
        hidden = (gate * sig * up).astype(jnp.bfloat16)
        expert_out = jnp.dot(hidden, down_w.T, preferred_element_type=jnp.float32).astype(jnp.bfloat16)
        out_grad = (weight[:, None] * cotan).astype(jnp.bfloat16)
        hidden_grad = jnp.dot(out_grad, down_w, preferred_element_type=jnp.float32)
        gate_term = (hidden_grad * up * sig * (1.0 + gate * (1.0 - sig))).astype(jnp.bfloat16)
        up_term = (hidden_grad * gate * sig).astype(jnp.bfloat16)
        slot_grad = (jnp.dot(gate_term, gate_w.T, preferred_element_type=jnp.float32)
                     + jnp.dot(up_term, up_w.T, preferred_element_type=jnp.float32)).astype(jnp.bfloat16)
        out_f = expert_out.astype(jnp.float32)
        out_acc = out_acc.at[token].add(weight[:, None] * out_f)
        grad_acc = grad_acc.at[token].add(slot_grad.astype(jnp.float32) * live[:, None])
        route_acc = route_acc.at[slot].add(jnp.sum(cotan * out_f, axis=1) * live)
        gate_g = jnp.dot(rows.T, gate_term, preferred_element_type=jnp.float32).astype(jnp.bfloat16)
        up_g = jnp.dot(rows.T, up_term, preferred_element_type=jnp.float32).astype(jnp.bfloat16)
        down_g = jnp.dot(out_grad.T, hidden, preferred_element_type=jnp.float32).astype(jnp.bfloat16)
        return (out_acc, grad_acc, route_acc), (gate_g, up_g, down_g)

    start = (jnp.zeros((TOKENS, D), jnp.float32), jnp.zeros((TOKENS, D), jnp.float32),
             jnp.zeros((slots,), jnp.float32))
    carry, grads = lax.scan(one_expert, start, jnp.arange(EXPERTS, dtype=jnp.int32))
    out_acc, grad_acc, route_acc = carry
    return (out_acc.astype(jnp.bfloat16), grad_acc.astype(jnp.bfloat16),
            route_acc.reshape(TOKENS, TOP), grads[0], grads[1], grads[2])
```

```python
import functools

import jax
import jax.numpy as jnp
from jax import lax
from jax.experimental import pallas as pl
from jax.experimental.pallas import tpu as pltpu
from jax.sharding import PartitionSpec as P

BF16 = jnp.bfloat16
F32 = jnp.float32
CORES = 2
VMEM_MAX = 60 * 1024 * 1024


def slot_table(expert_ids, experts, capacity):
    flat = expert_ids.reshape(-1)
    count = flat.shape[0]
    same = flat[:, None] == flat[None, :]
    earlier = lax.broadcasted_iota(jnp.int32, (count, count), 0) > lax.broadcasted_iota(
        jnp.int32, (count, count), 1
    )
    rank = jnp.sum((same & earlier).astype(jnp.int32), axis=1)
    target = flat * capacity + rank
    columns = lax.broadcasted_iota(jnp.int32, (count, experts * capacity), 1)
    return (target[:, None] == columns).astype(jnp.bfloat16)


def contract_last(left, right):
    return lax.dot_general(
        left, right, (((1,), (1,)), ((), ())), preferred_element_type=jnp.float32
    )


def contract_first(left, right):
    return lax.dot_general(
        left, right, (((0,), (0,)), ((), ())), preferred_element_type=jnp.float32
    )


def expert_forward(rows, gate_w, up_w, down_w):
    gate = jnp.dot(rows, gate_w, preferred_element_type=jnp.float32)
    up = jnp.dot(rows, up_w, preferred_element_type=jnp.float32)
    sig = jax.nn.sigmoid(gate)
    hidden = (gate * sig * up).astype(jnp.bfloat16)
    expert_out = contract_last(hidden, down_w).astype(jnp.bfloat16)
    return (expert_out, (gate, up, sig, hidden))


def expert_backward(out_grad, saved, gate_w, up_w, down_w):
    gate, up, sig, hidden = saved
    hidden_grad = jnp.dot(out_grad, down_w, preferred_element_type=jnp.float32)
    gate_term = (hidden_grad * up * sig * (1.0 + gate * (1.0 - sig))).astype(jnp.bfloat16)
    up_term = (hidden_grad * gate * sig).astype(jnp.bfloat16)
    slot_grad = (contract_last(gate_term, gate_w) + contract_last(up_term, up_w)).astype(
        jnp.bfloat16
    )
    return (slot_grad, gate_term, up_term)


def weight_grads(rows, out_grad, gate_term, up_term, hidden):
    part_rows, part_grad = (
        lax.all_to_all(rows, "dp", split_axis=1, concat_axis=0, tiled=True),
        lax.all_to_all(out_grad, "dp", split_axis=1, concat_axis=0, tiled=True),
    )
    all_gate, all_up, all_hidden = (
        lax.all_gather(gate_term, "dp", axis=0, tiled=True),
        lax.all_gather(up_term, "dp", axis=0, tiled=True),
        lax.all_gather(hidden, "dp", axis=0, tiled=True),
    )
    down_g = contract_first(part_grad, all_hidden).astype(jnp.bfloat16)
    gate_g = contract_first(part_rows, all_gate).astype(jnp.bfloat16)
    up_g = contract_first(part_rows, all_up).astype(jnp.bfloat16)
    return (gate_g, up_g, down_g)


def body(tokens, expert_ids, route_weights, w_gate, w_up, w_down, grad_out):
    local = w_gate.shape[0]
    groups = lax.axis_size("expert")
    experts = local * groups
    count = tokens.shape[0]
    top = expert_ids.shape[1]
    width = tokens.shape[1]
    capacity = max(2, (3 * count * top + 2 * experts - 1) // (2 * experts))
    table = slot_table(expert_ids, experts, capacity)
    per_token = jnp.sum(table.reshape(count, top, experts * capacity), axis=1)
    send_rows = jnp.dot(per_token.T, tokens, preferred_element_type=jnp.float32)
    send_rows = send_rows.astype(jnp.bfloat16).reshape(experts, capacity, width)
    weighted = (route_weights[:, :, None] * grad_out.astype(jnp.float32)[:, None, :]).astype(
        jnp.bfloat16
    )
    send_grad = jnp.dot(
        table.T, weighted.reshape(count * top, width), preferred_element_type=jnp.float32
    )
    send_grad = send_grad.astype(jnp.bfloat16).reshape(experts, capacity, width)
    full_gate, full_up, full_down = (
        lax.all_gather(w_gate, "dp", axis=1, tiled=True),
        lax.all_gather(w_up, "dp", axis=1, tiled=True),
        lax.all_gather(w_down, "dp", axis=1, tiled=True),
    )
    received = lax.all_to_all(send_rows, "expert", split_axis=0, concat_axis=0, tiled=True)
    shaped = received.reshape(groups, local, capacity, width)
    saves = []
    inputs = []
    slot_expert = 0
    rows = shaped[:, slot_expert].reshape(groups * capacity, width)
    expert_out, saved = expert_forward(
        rows, full_gate[slot_expert], full_up[slot_expert], full_down[slot_expert]
    )
    outs = expert_out.reshape(groups, 1, capacity, width)
    saves.append(saved)
    inputs.append(rows)
    expert_outs, saves, inputs = (outs.reshape(experts, capacity, width), saves, inputs)
    back_out = lax.all_to_all(expert_outs, "expert", split_axis=0, concat_axis=0, tiled=True)
    received_grad = lax.all_to_all(send_grad, "expert", split_axis=0, concat_axis=0, tiled=True)
    shaped = received_grad.reshape(groups, local, capacity, width)
    slot_expert = 0
    out_grad = shaped[:, slot_expert].reshape(groups * capacity, width)
    slot_grad, gate_term, up_term = expert_backward(
        out_grad,
        saves[slot_expert],
        full_gate[slot_expert],
        full_up[slot_expert],
        full_down[slot_expert],
    )
    grads_in = slot_grad.reshape(groups, 1, capacity, width)
    gate_g, up_g, down_g = weight_grads(
        inputs[slot_expert], out_grad, gate_term, up_term, saves[slot_expert][3]
    )
    gate_list = [gate_g]
    up_list = [up_g]
    down_list = [down_g]
    slot_grads = grads_in.reshape(experts, capacity, width)
    gate_grad = jnp.stack(gate_list)
    up_grad = jnp.stack(up_list)
    down_grad = jnp.stack(down_list)
    back_grad = lax.all_to_all(slot_grads, "expert", split_axis=0, concat_axis=0, tiled=True)
    out_slots = jnp.dot(
        table, back_out.reshape(experts * capacity, width), preferred_element_type=jnp.float32
    )
    out_slots = out_slots.reshape(count, top, width)
    layer_out = jnp.sum(route_weights[:, :, None] * out_slots, axis=1).astype(jnp.bfloat16)
    route_grad = jnp.sum(grad_out.astype(jnp.float32)[:, None, :] * out_slots, axis=2)
    grad_slots = jnp.dot(
        table, back_grad.reshape(experts * capacity, width), preferred_element_type=jnp.float32
    )
    token_grad = jnp.sum(grad_slots.reshape(count, top, width), axis=1).astype(jnp.bfloat16)
    return (layer_out, token_grad, route_grad, gate_grad, up_grad, down_grad)


def pad16(n):
    return (n + 15) // 16 * 16


def prefix_count(member):
    t = member.shape[1]
    before = lax.broadcasted_iota(jnp.int32, (t, t), 0) < lax.broadcasted_iota(jnp.int32, (t, t), 1)
    return jnp.sum(member[:, :, None] * before.astype(F32)[None], axis=1)


def route_tables(expert_ids, route_weights, groups):
    count, top = expert_ids.shape
    stages = groups // CORES
    chip = lax.axis_index("expert") // CORES
    lanes = lax.broadcasted_iota(jnp.int32, (count,), 0)
    experts = lax.broadcasted_iota(jnp.int32, (groups, count), 0)
    member = jnp.zeros((groups, count), F32)
    weight = jnp.zeros((groups, count), F32)
    for k in range(top):
        hit = (expert_ids[:, k][None, :] == experts).astype(F32)
        member = member + hit
        weight = weight + hit * route_weights[:, k][None, :]
    slot = jnp.where(member > 0, prefix_count(member), -1.0)

    def position(first):
        key = jnp.where(first, lanes, lanes + count)
        return jnp.sum((key[:, None] < key[None, :]).astype(F32), axis=0)

    pos_up = position(jnp.any(expert_ids // CORES == stages - 1, axis=1))
    pos_down = position(jnp.any(expert_ids // CORES == 0, axis=1))
    dest = lax.broadcasted_iota(jnp.int32, (groups, 1), 0) // CORES
    pos = jnp.where(dest >= chip, pos_up[None, :], pos_down[None, :])
    pick = (pos[:, None, :] == lanes.astype(F32)[None, :, None]).astype(F32)
    slot_rows = jnp.sum(pick * slot[:, None, :], axis=2)
    weight_rows = jnp.sum(pick * weight[:, None, :], axis=2)
    swap = lambda a: a.reshape(stages, CORES, count)[:, ::-1].reshape(groups, count)
    zero = jnp.zeros_like(slot)
    meta = jnp.stack(
        [slot_rows, weight_rows, swap(slot_rows), slot, swap(slot), zero, zero, zero], axis=1
    )
    order = jnp.stack([pos_up, pos_down] + [jnp.zeros_like(pos_up)] * 6, axis=0)
    return meta, order


def one_hot(row, height):
    rows = lax.broadcasted_iota(jnp.int32, (height, row.shape[1]), 0).astype(F32)
    return (rows == row).astype(F32)


def choose(index, values):
    result = jnp.int32(values[0])
    for i in range(1, len(values)):
        result = jnp.where(index == i, jnp.int32(values[i]), result)
    return result


def visit_order(chip, stages):
    inner = -1 if 2 * chip >= stages else 1
    near = [s for d in range(stages) for s in ((chip + d * inner, chip - d * inner) if d else (chip,))]
    return [s for s in near if 0 <= s < stages]


def moe_kernel(
    groups, ndp, cap, edge,
    tok_hbm, grad_hbm, meta_ref, order_ref, wg_hbm, wu_hbm, wd_hbm,
    out_hbm, tgrad_hbm, route_ref, gg_hbm, ug_hbm, dg_hbm,
    tok, grad, blocks, own_down, metas, xr, gr, wr, wgu, wd, yy, ym, ret_in, ret_down, ret_out,
    fa, fb, hid, hs, both, dots, gs, gs2, grx, keep, own, gout, route_out, route_in,
    in_send, in_recv, meta_send, meta_recv, w_send, w_recv, pc_send, pc_recv,
    ret_send, ret_recv, retd_recv, route_send, route_recv, gr_send, gr_recv, load_sem, store_sem,
):
    stages = groups // CORES
    count, width = tok.shape
    part, ff = gout.shape[1:]
    half, hp = count // 2, part // 2
    me = lax.axis_index("expert")
    dp = lax.axis_index("dp")
    chip, core = me // CORES, me % CORES
    mate = chip * CORES + (1 - core)
    px, py = dp % 2, dp // 2
    xn, yn, dg = py * 2 + (1 - px), (1 - py) * 2 + px, (1 - py) * 2 + (1 - px)
    to_mate, to_x, to_y = {"expert": mate}, {"dp": xn}, {"dp": yn}
    at_edge = (chip == 0) | (chip == stages - 1)
    inside = jnp.logical_not(at_edge)
    has_up, has_down = chip < stages - 1, chip > 0
    up_dev, down_dev = {"expert": me + CORES}, {"expert": me - CORES}
    low = 2 * chip < stages
    yes = chip >= 0
    pending = []

    def copy(src, dst, ssem, rsem, where):
        return pltpu.make_async_remote_copy(
            src_ref=src, dst_ref=dst, send_sem=ssem, recv_sem=rsem,
            device_id=where, device_id_type=pl.DeviceIdType.MESH,
        )

    def send(cond, *args):
        if cond is None:
            copy(*args).start()
        else:
            pl.when(cond)(lambda: copy(*args).start())
        pending.append((cond, args))

    def landed(ref, sem):
        copy(ref, ref, sem, sem, to_mate).wait_recv()

    def rows_of(c, short):
        end = half if c == 0 else (edge if short else count)
        return pl.ds(c * half, end - c * half)

    def send_rows(cond, short, c, src, dst, ssem, rsem, where):
        if c == 0 or edge == count:
            send(cond, src.at[rows_of(c, False)], dst.at[rows_of(c, False)], ssem, rsem, where)
            return
        full = jnp.logical_not(short)
        if cond is not None:
            short, full = cond & short, cond & full
        for when, cut in ((full, rows_of(c, False)), (short, rows_of(c, True))):
            send(when, src.at[cut], dst.at[cut], ssem, rsem, where)

    def wait_rows(cond, short, c, dst, sem):
        if c == 0 or edge == count:
            pl.when(cond)(lambda: landed(dst.at[rows_of(c, False)], sem))
            return
        pl.when(cond & jnp.logical_not(short))(lambda: landed(dst.at[rows_of(c, False)], sem))
        pl.when(cond & short)(lambda: landed(dst.at[rows_of(c, True)], sem))

    def nt(a, b):
        return lax.dot_general(a, b, (((1,), (1,)), ((), ())), preferred_element_type=F32)

    def tn(a, b):
        return lax.dot_general(a, b, (((0,), (0,)), ((), ())), preferred_element_type=F32)

    def nn(a, b):
        return jnp.dot(a, b, preferred_element_type=F32)

    gate_cols, up_cols = pl.ds(0, ff), pl.ds(ff, ff)

    def weight(i, j):
        return wd.at[j] if i == 2 else wgu.at[j, :, gate_cols if i == 0 else up_cols]

    loads = [
        pltpu.make_async_copy(src, dst, load_sem.at[n])
        for n, (src, dst) in enumerate((
            (tok_hbm, tok), (wg_hbm, weight(0, dp)), (wu_hbm, weight(1, dp)), (grad_hbm, grad),
            (wd_hbm, weight(2, dp)),
        ))
    ]
    for load in loads:
        load.start()

    if edge < count:
        rest = pl.ds(edge, count - edge)
        empty = jnp.zeros((count - edge, width), BF16)
        for t in range(2):
            for s in range(stages):
                blocks[0, t, s, rest] = empty
                blocks[1, t, s, rest] = empty
                ret_in[t, s, rest] = empty
            ret_down[t, rest] = empty
    for t in range(2):
        @pl.when(chip == stages - 1)
        def _():
            ret_in[t, chip] = jnp.zeros((count, width), BF16)

        @pl.when(chip == 0)
        def _():
            ret_down[t] = jnp.zeros((count, width), BF16)

    up_hot = one_hot(order_ref[0:1, :], count).astype(BF16)
    down_hot = one_hot(order_ref[1:2, :], count).astype(BF16)
    metas[me] = meta_ref[me]

    def arrange(t):
        value = (tok, grad)[t][...]
        blocks[0, t, chip] = nn(up_hot, value).astype(BF16)
        own_down[t] = nn(down_hot, value).astype(BF16)

    loads[0].wait()
    arrange(0)

    barrier = pltpu.get_barrier_semaphore()
    for off in range(1, groups):
        pl.semaphore_signal(barrier, inc=1, device_id={"expert": (me + off) % groups},
                            device_id_type=pl.DeviceIdType.MESH)
    for off in range(1, ndp):
        pl.semaphore_signal(barrier, inc=1, device_id={"dp": (dp + off) % ndp},
                            device_id_type=pl.DeviceIdType.MESH)
    pl.semaphore_wait(barrier, groups + ndp - 2)

    def depart_up(t, cond):
        for c in range(2):
            send_rows(cond, chip + 1 == stages - 1, c, blocks.at[0, t, chip], blocks.at[0, t, chip],
                      in_send.at[t, 0, 0, c], in_recv.at[0, t, chip, c], up_dev)

    def depart_down(t, cond):
        for c in range(2):
            send_rows(cond, chip - 1 == 0, c, own_down.at[t], blocks.at[0, t, chip],
                      in_send.at[t, 0, 1, c], in_recv.at[0, t, chip, c], down_dev)

    def depart_mate(t):
        send(None, blocks.at[0, t, chip], blocks.at[1, t, chip],
             in_send.at[t, 0, 2, 0], in_recv.at[1, t, chip, 0], to_mate)

    halves = (pl.ds(0, hp), pl.ds(hp, hp))

    def weight_direct(i):
        for n, (h, where) in enumerate(((0, to_x), (1, to_y), (1, to_x), (0, to_y))):
            ref = weight(i, dp).at[halves[h]]
            send(None, ref, ref, w_send.at[i, n], w_recv.at[i, n], where)

    def weight_relay(i):
        for n, (h, j, where) in enumerate(((0, xn, to_y), (1, yn, to_x))):
            ref = weight(i, j).at[halves[h]]
            landed(ref, w_recv.at[i, n])
            send(None, ref, ref, w_send.at[i, 4 + n], w_recv.at[i, 4 + n], where)

    def weight_rest(i):
        for n, (h, j) in ((2, (1, xn)), (3, (0, yn)), (4, (0, dg)), (5, (1, dg))):
            landed(weight(i, j).at[halves[h]], w_recv.at[i, n])

    depart_up(0, has_up)
    depart_down(0, has_down)
    depart_mate(0)
    for off in range(1, groups):
        other = (me + off) % groups
        send(None, meta_ref.at[other], metas.at[me], meta_send.at[off - 1], meta_recv.at[off - 1],
             {"expert": other})
    for i in range(2):
        loads[1 + i].wait()
        weight_direct(i)
    loads[3].wait()
    arrange(1)
    depart_up(1, has_up & at_edge)
    depart_down(1, has_down & at_edge)
    depart_mate(1)
    for off in range(1, groups):
        copy(meta_ref.at[0], metas.at[0], meta_send.at[off - 1], meta_recv.at[off - 1],
             to_mate).wait_recv()

    table = [visit_order(z, stages) for z in range(stages)]
    source = [choose(chip, [table[z][q] for z in range(stages)]) for q in range(stages)]

    def arrive(t, q, c):
        s = source[q]
        nxt = jnp.where(s < chip, chip + 1, chip - 1)
        more = (nxt >= 0) & (nxt < stages)
        wait_rows(yes, at_edge, c, blocks.at[0, t, s], in_recv.at[0, t, s, c])
        send_rows(more, (nxt == 0) | (nxt == stages - 1), c, blocks.at[0, t, s],
                  blocks.at[0, t, s], in_send.at[t, q, 0, c], in_recv.at[0, t, s, c],
                  {"expert": nxt * CORES + core})
        send_rows(None, at_edge, c, blocks.at[0, t, s], blocks.at[1, t, s],
                  in_send.at[t, q, 2, c], in_recv.at[1, t, s, c], to_mate)

    def compact(t, q):
        s = source[q]
        for r in range(2):
            if r == 1 and q == 0:
                landed(blocks.at[1, t, s], in_recv.at[1, t, s, 0])
            elif r == 1:
                for c in range(2):
                    wait_rows(yes, at_edge, c, blocks.at[1, t, s], in_recv.at[1, t, s, c])
            tile = metas[s * CORES + (core if r == 0 else 1 - core)]
            hot = one_hot(tile[0:1, :], cap)
            rows = pl.ds((q * 2 + r) * cap, cap)
            (xr, gr)[t][rows, :] = nn(hot.astype(BF16), blocks[r, t, s]).astype(BF16)
            if t == 0:
                scale = jnp.sum(hot * tile[1:2, :], axis=1, keepdims=True)
                wr[rows, :] = jnp.broadcast_to(scale, (cap, 128))

    compact(0, 0)
    near = range(1, stages - 1)
    last = stages - 1
    for q in near:
        arrive(0, q, 0)
    for i in range(2):
        weight_relay(i)
    loads[4].wait()
    weight_direct(2)
    for q in near:
        arrive(0, q, 1)
    for q in near:
        compact(0, q)
    arrive(0, last, 0)
    depart_up(1, inside & low)
    depart_down(1, inside & jnp.logical_not(low))
    arrive(0, last, 1)
    depart_up(1, inside & jnp.logical_not(low))
    depart_down(1, inside & low)
    compact(0, last)
    for i in range(2):
        weight_rest(i)

    def cut(j):
        return pl.ds(j * part, part)

    def cut_at(j):
        return pl.ds(pl.multiple_of(j * part, part), part)

    total = xr.shape[0]
    gu = jnp.zeros((total, 2 * ff), F32)
    for j in range(ndp):
        gu += nn(xr[:, cut(j)], wgu[j])
    gate, up = gu[:, :ff], gu[:, ff:]
    sig = jax.nn.sigmoid(gate)
    scale = wr[:, 0:1]
    gated = gate * sig
    value = gated * up
    hid[...] = value.astype(BF16)
    hs[...] = (scale * value).astype(BF16)
    fa[...] = scale * (up * sig * (1.0 + gate * (1.0 - sig)))
    fb[...] = scale * gated

    for q in near:
        arrive(1, q, 0)
    weight_relay(2)
    for q in near:
        arrive(1, q, 1)
    for q in range(last):
        compact(1, q)

    def place(t, cols, value, qs):
        for n, q in enumerate(qs):
            yy[t, q, 0:cap, cols] = value[2 * n * cap:(2 * n + 1) * cap]
            ym[t, q, :, cols] = value[(2 * n + 1) * cap:(2 * n + 2) * cap]

    def pair(t, qs):
        for q in reversed(qs):
            send(None, ym.at[t, q], yy.at[t, q, pl.ds(cap, cap)], pc_send.at[t, q],
                 pc_recv.at[t, q], to_mate)

    everyone = range(stages)
    for n, j in enumerate((dp, xn, yn, dg)):
        if n == 1:
            weight_rest(2)
        place(0, cut_at(j), nt(hs[...], wd[j]).astype(BF16), everyone)
    pair(0, everyone)

    def expand(t, q, c, row_own, row_mate):
        tile = metas[source[q] * CORES + core]
        hot = jnp.concatenate(
            [one_hot(tile[row_own:row_own + 1, :], cap), one_hot(tile[row_mate:row_mate + 1, :], cap)],
            axis=0).astype(BF16)
        if c is not None:
            hot = hot[:, c * half:(c + 1) * half]
        return tn(hot, yy[t, q])

    def give_back(t, q, ends):
        s = source[q]
        rising = s > chip
        nxt = jnp.where(rising, chip + 1, chip - 1)
        back = jnp.where(rising, chip - 1, chip + 1)
        where = {"expert": nxt * CORES + core}
        here = at_edge if ends else inside
        arrives = rising & (nxt == s)
        pl.when(here)(lambda: landed(yy.at[t, q, pl.ds(cap, cap)], pc_recv.at[t, q]))
        for c in range(2):
            lines = pl.ds(c * half, half)
            if not ends:
                wait_rows(here, (back == 0) | (back == stages - 1), c, ret_in.at[t, s],
                          ret_recv.at[t, s, c])

            @pl.when(here)
            def _():
                value = expand(t, q, c, 0, 2)
                if not ends:
                    value = value + ret_in[t, s, lines].astype(F32)
                ret_out[t, q, lines] = value.astype(BF16)

            rows = rows_of(c, ends)
            send(here & arrives, ret_out.at[t, q, rows], ret_down.at[t, rows], ret_send.at[t, q, c],
                 retd_recv.at[t, c], where)
            send(here & jnp.logical_not(arrives), ret_out.at[t, q, rows], ret_in.at[t, s, rows],
                 ret_send.at[t, q, c], ret_recv.at[t, s, c], where)

    def backward(qs):
        rows = pl.ds(qs[0] * 2 * cap, len(qs) * 2 * cap)
        hg = nn(gr[rows, cut(0)], wd[0])
        for j in range(1, ndp):
            hg += nn(gr[rows, cut(j)], wd[j])
        both[rows, :ff] = (hg * fa[rows, :]).astype(BF16)
        both[rows, ff:] = (hg * fb[rows, :]).astype(BF16)
        line = jnp.sum(hg * hid[rows, :].astype(F32), axis=1, keepdims=True)
        dots[rows, :] = jnp.broadcast_to(line, (line.shape[0], 128))
        for j in range(ndp):
            place(1, cut(j), nt(both[rows, :], wgu[j]).astype(BF16), qs)
        pair(1, qs)

    give_back(0, last, True)
    for q in reversed(near):
        if q > 1:
            give_back(0, q, True)
    arrive(1, last, 0)
    backward(range(last))
    arrive(1, last, 1)
    compact(1, last)
    backward(range(last, stages))

    def weight_slice(j):
        cols = cut_at(j)
        return nn_t(xr, cols, both), nn_t(gr, cols, hs)

    def nn_t(rows_ref, cols, ref):
        return tn(rows_ref[:, cols], ref[...])

    def pieces(value, down, h):
        top = slice(h * hp, (h + 1) * hp)
        return value[top, :ff], value[top, ff:], down[top]

    def give_grad(k, h, values, where):
        for i, v in enumerate(pieces(*values, h)):
            gs[i, k] = v.astype(BF16)
        for i in range(3):
            send(None, gs.at[i, k], grx.at[i, k], gr_send.at[i, k], gr_recv.at[i, k], where)

    def keep_grad(k, h, values):
        for i, v in enumerate(pieces(*values, h)):
            keep[i, k] = v

    values = weight_slice(dg)
    give_grad(0, 0, values, to_x)
    give_grad(1, 1, values, to_y)
    give_back(0, last, False)
    give_back(1, last, True)
    values = weight_slice(xn)
    give_grad(2, 0, values, to_x)
    keep_grad(1, 1, values)
    values = weight_slice(yn)
    give_grad(3, 1, values, to_y)
    keep_grad(0, 0, values)
    for q in near:
        give_back(0, q, False)
    for q in reversed(near):
        if q > 1:
            give_back(1, q, True)
    for t in range(2):
        give_back(t, 1, True)

    for q in range(stages):
        for r in range(2):
            origin = source[q] * CORES + (core if r == 0 else 1 - core)
            hot = one_hot(metas[origin][3:4, :], cap)
            part_dots = dots[(q * 2 + r) * cap:(q * 2 + r + 1) * cap, 0:1]
            line = jnp.sum(hot * part_dots, axis=0, keepdims=True)
            route_out[origin] = jnp.broadcast_to(line, (8, count))
    for off in range(1, groups):
        other = (me + off) % groups
        send(None, route_out.at[other], route_in.at[me], route_send.at[off - 1],
             route_recv.at[off - 1], {"expert": other})
    route_in[me] = route_out[me]

    values = weight_slice(dp)
    for h in range(2):
        for i, v in enumerate(pieces(*values, h)):
            own[i, h] = v

    give_back(1, last, False)
    for i in range(3):
        for k, where in ((0, to_y), (1, to_x)):
            landed(grx.at[i, k], gr_recv.at[i, k])
            gs2[i, k] = (keep[i, k] + grx[i, k].astype(F32)).astype(BF16)
            send(None, gs2.at[i, k], grx.at[i, 4 + k], gr_send.at[i, 4 + k], gr_recv.at[i, 4 + k],
                 where)
    for q in near:
        give_back(1, q, False)

    stores = []

    def store(src, dst):
        cp = pltpu.make_async_copy(src, dst, store_sem.at[len(stores)])
        cp.start()
        stores.append(cp)

    for t, (ref, hbm) in enumerate(((tok, out_hbm), (grad, tgrad_hbm))):
        landed(yy.at[t, 0, pl.ds(cap, cap)], pc_recv.at[t, 0])
        value = expand(t, 0, None, 3, 4)
        for c in range(2):
            wait_rows(has_up, chip + 1 == stages - 1, c, ret_in.at[t, chip], ret_recv.at[t, chip, c])
            wait_rows(has_down, chip - 1 == 0, c, ret_down.at[t], retd_recv.at[t, c])
        value += tn(up_hot, ret_in[t, chip]) + tn(down_hot, ret_down[t])
        ref[...] = value.astype(BF16)
        store(ref, hbm)

    for off in range(1, groups):
        copy(route_out.at[0], route_in.at[0], route_send.at[off - 1], route_recv.at[off - 1],
             to_mate).wait_recv()
    route_ref[...] = route_in[...]
    for i, hbm in enumerate((gg_hbm, ug_hbm, dg_hbm)):
        for h in range(2):
            value = own[i, h]
            for k in (2 + h, 4 + h):
                landed(grx.at[i, k], gr_recv.at[i, k])
                value += grx[i, k].astype(F32)
            gout[i, halves[h]] = value.astype(BF16)
        store(gout.at[i], hbm)
    for cond, args in pending:
        if cond is None:
            copy(*args).wait_send()
        else:
            pl.when(cond)(lambda args=args: copy(*args).wait_send())
    for cp in stores:
        cp.wait()


def kernel_scratch(groups, ndp, cap, count, width, part, ff):
    stages = groups // CORES
    rows = groups * cap
    hp = part // 2
    shapes = [
        ((count, width), BF16),
        ((count, width), BF16),
        ((2, 2, stages, count, width), BF16),
        ((2, count, width), BF16),
        ((groups, 8, count), F32),
        ((rows, width), BF16),
        ((rows, width), BF16),
        ((rows, 128), F32),
        ((ndp, part, 2 * ff), BF16),
        ((ndp, part, ff), BF16),
        ((2, stages, 2 * cap, width), BF16),
        ((2, stages, cap, width), BF16),
        ((2, stages, count, width), BF16),
        ((2, count, width), BF16),
        ((2, stages, count, width), BF16),
        ((rows, ff), F32),
        ((rows, ff), F32),
        ((rows, ff), BF16),
        ((rows, ff), BF16),
        ((rows, 2 * ff), BF16),
        ((rows, 128), F32),
        ((3, 4, hp, ff), BF16),
        ((3, 2, hp, ff), BF16),
        ((3, 6, hp, ff), BF16),
        ((3, 2, hp, ff), F32),
        ((3, 2, hp, ff), F32),
        ((3, part, ff), BF16),
        ((groups, 8, count), F32),
        ((groups, 8, count), F32),
    ]
    sems = [
        (2, stages, 3, 2), (2, 2, stages, 2), (groups - 1,), (groups - 1,), (3, 6), (3, 6),
        (2, stages), (2, stages), (2, stages, 2), (2, stages, 2), (2, 2), (groups - 1,),
        (groups - 1,), (3, 6), (3, 6), (5,), (5,),
    ]
    return shapes, sems


def scratch_bytes(shapes):
    total = 0
    for shape, dtype in shapes:
        size = jnp.dtype(dtype).itemsize
        for n in shape:
            size *= n
        total += size
    return total


def slot_capacity(count, top, experts):
    return max(2, (3 * count * top + 2 * experts - 1) // (2 * experts))


def line_body(groups, ndp, tokens, expert_ids, route_weights, w_gate, w_up, w_down, grad_out):
    count, width = tokens.shape
    _, part, ff = w_gate.shape
    top = expert_ids.shape[1]
    slots = slot_capacity(count, top, groups)
    cap = pad16(slots)
    edge = min(count, pad16(CORES * slots))
    meta, order = route_tables(expert_ids, route_weights, groups)
    shapes, sems = kernel_scratch(groups, ndp, cap, count, width, part, ff)
    vmem = pl.BlockSpec(memory_space=pltpu.VMEM)
    hbm = pl.BlockSpec(memory_space=pl.ANY)
    layer_out, token_grad, route, gate_g, up_g, down_g = pl.pallas_call(
        functools.partial(moe_kernel, groups, ndp, cap, edge),
        out_shape=(
            jax.ShapeDtypeStruct((count, width), BF16),
            jax.ShapeDtypeStruct((count, width), BF16),
            jax.ShapeDtypeStruct((groups, 8, count), F32),
            jax.ShapeDtypeStruct((part, ff), BF16),
            jax.ShapeDtypeStruct((part, ff), BF16),
            jax.ShapeDtypeStruct((part, ff), BF16),
        ),
        in_specs=[hbm, hbm, vmem, vmem, hbm, hbm, hbm],
        out_specs=(hbm, hbm, vmem, hbm, hbm, hbm),
        scratch_shapes=[pltpu.VMEM(s, d) for s, d in shapes]
        + [pltpu.SemaphoreType.DMA(s) for s in sems],
        compiler_params=pltpu.CompilerParams(
            collective_id=0, has_side_effects=True, vmem_limit_bytes=VMEM_MAX
        ),
    )(tokens, grad_out, meta, order, w_gate[0], w_up[0], w_down[0])
    experts = lax.broadcasted_iota(jnp.int32, (groups, count, top), 0)
    mine = (expert_ids[None] == experts).astype(F32)
    route_grad = jnp.sum(mine * route[:, 0, :, None], axis=0)
    return layer_out, token_grad, route_grad, gate_g[None], up_g[None], down_g[None]


def pick_body(groups, ndp, *args):
    tokens, expert_ids, _, w_gate = args[:4]
    count, width = tokens.shape
    local, part, ff = w_gate.shape
    if local == 1 and groups == 4 * CORES and ndp == 4:
        slots = slot_capacity(count, expert_ids.shape[1], groups)
        shapes, _ = kernel_scratch(groups, ndp, pad16(slots), count, width, part, ff)
        tiled = count % 32 == 0 and part % 128 == 0 and ff % 128 == 0 and 4 * slots > count
        if tiled and scratch_bytes(shapes) < VMEM_MAX * 9 // 10:
            return line_body(groups, ndp, *args)
    return body(*args)


def solution(mesh):
    in_specs = (
        P(("dp", "expert"), None),
        P(("dp", "expert"), None),
        P(("dp", "expert"), None),
        P("expert", "dp", None),
        P("expert", "dp", None),
        P("expert", "dp", None),
        P(("dp", "expert"), None),
    )
    out_specs = (
        P(("dp", "expert"), None),
        P(("dp", "expert"), None),
        P(("dp", "expert"), None),
        P("expert", "dp", None),
        P("expert", "dp", None),
        P("expert", "dp", None),
    )
    step = functools.partial(pick_body, mesh.shape["expert"], mesh.shape["dp"])
    return jax.shard_map(step, mesh=mesh, in_specs=in_specs, out_specs=out_specs, check_vma=False)
```

```python
import functools

import jax
import jax.numpy as jnp
from jax import lax
from jax.experimental import pallas as pl
from jax.experimental.pallas import tpu as pltpu
from jax.sharding import PartitionSpec as P

BF16 = jnp.bfloat16
F32 = jnp.float32
CORES = 2
VMEM_MAX = 56 * 1024 * 1024


def slot_table(expert_ids, experts, capacity):
    flat = expert_ids.reshape(-1)
    count = flat.shape[0]
    same = flat[:, None] == flat[None, :]
    earlier = lax.broadcasted_iota(jnp.int32, (count, count), 0) > lax.broadcasted_iota(
        jnp.int32, (count, count), 1
    )
    rank = jnp.sum((same & earlier).astype(jnp.int32), axis=1)
    target = flat * capacity + rank
    columns = lax.broadcasted_iota(jnp.int32, (count, experts * capacity), 1)
    return (target[:, None] == columns).astype(jnp.bfloat16)


def contract_last(left, right):
    return lax.dot_general(
        left, right, (((1,), (1,)), ((), ())), preferred_element_type=jnp.float32
    )


def contract_first(left, right):
    return lax.dot_general(
        left, right, (((0,), (0,)), ((), ())), preferred_element_type=jnp.float32
    )


def expert_forward(rows, gate_w, up_w, down_w):
    gate = jnp.dot(rows, gate_w, preferred_element_type=jnp.float32)
    up = jnp.dot(rows, up_w, preferred_element_type=jnp.float32)
    sig = jax.nn.sigmoid(gate)
    hidden = (gate * sig * up).astype(jnp.bfloat16)
    expert_out = contract_last(hidden, down_w).astype(jnp.bfloat16)
    return (expert_out, (gate, up, sig, hidden))


def expert_backward(out_grad, saved, gate_w, up_w, down_w):
    gate, up, sig, hidden = saved
    hidden_grad = jnp.dot(out_grad, down_w, preferred_element_type=jnp.float32)
    gate_term = (hidden_grad * up * sig * (1.0 + gate * (1.0 - sig))).astype(jnp.bfloat16)
    up_term = (hidden_grad * gate * sig).astype(jnp.bfloat16)
    slot_grad = (contract_last(gate_term, gate_w) + contract_last(up_term, up_w)).astype(
        jnp.bfloat16
    )
    return (slot_grad, gate_term, up_term)


def weight_grads(rows, out_grad, gate_term, up_term, hidden):
    part_rows, part_grad = (
        lax.all_to_all(rows, "dp", split_axis=1, concat_axis=0, tiled=True),
        lax.all_to_all(out_grad, "dp", split_axis=1, concat_axis=0, tiled=True),
    )
    all_gate, all_up, all_hidden = (
        lax.all_gather(gate_term, "dp", axis=0, tiled=True),
        lax.all_gather(up_term, "dp", axis=0, tiled=True),
        lax.all_gather(hidden, "dp", axis=0, tiled=True),
    )
    down_g = contract_first(part_grad, all_hidden).astype(jnp.bfloat16)
    gate_g = contract_first(part_rows, all_gate).astype(jnp.bfloat16)
    up_g = contract_first(part_rows, all_up).astype(jnp.bfloat16)
    return (gate_g, up_g, down_g)


def body(tokens, expert_ids, route_weights, w_gate, w_up, w_down, grad_out):
    local = w_gate.shape[0]
    groups = lax.axis_size("expert")
    experts = local * groups
    count = tokens.shape[0]
    top = expert_ids.shape[1]
    width = tokens.shape[1]
    capacity = max(2, (3 * count * top + 2 * experts - 1) // (2 * experts))
    table = slot_table(expert_ids, experts, capacity)
    per_token = jnp.sum(table.reshape(count, top, experts * capacity), axis=1)
    send_rows = jnp.dot(per_token.T, tokens, preferred_element_type=jnp.float32)
    send_rows = send_rows.astype(jnp.bfloat16).reshape(experts, capacity, width)
    weighted = (route_weights[:, :, None] * grad_out.astype(jnp.float32)[:, None, :]).astype(
        jnp.bfloat16
    )
    send_grad = jnp.dot(
        table.T, weighted.reshape(count * top, width), preferred_element_type=jnp.float32
    )
    send_grad = send_grad.astype(jnp.bfloat16).reshape(experts, capacity, width)
    full_gate, full_up, full_down = (
        lax.all_gather(w_gate, "dp", axis=1, tiled=True),
        lax.all_gather(w_up, "dp", axis=1, tiled=True),
        lax.all_gather(w_down, "dp", axis=1, tiled=True),
    )
    received = lax.all_to_all(send_rows, "expert", split_axis=0, concat_axis=0, tiled=True)
    shaped = received.reshape(groups, local, capacity, width)
    saves = []
    inputs = []
    slot_expert = 0
    rows = shaped[:, slot_expert].reshape(groups * capacity, width)
    expert_out, saved = expert_forward(
        rows, full_gate[slot_expert], full_up[slot_expert], full_down[slot_expert]
    )
    outs = expert_out.reshape(groups, 1, capacity, width)
    saves.append(saved)
    inputs.append(rows)
    expert_outs, saves, inputs = (outs.reshape(experts, capacity, width), saves, inputs)
    back_out = lax.all_to_all(expert_outs, "expert", split_axis=0, concat_axis=0, tiled=True)
    received_grad = lax.all_to_all(send_grad, "expert", split_axis=0, concat_axis=0, tiled=True)
    shaped = received_grad.reshape(groups, local, capacity, width)
    slot_expert = 0
    out_grad = shaped[:, slot_expert].reshape(groups * capacity, width)
    slot_grad, gate_term, up_term = expert_backward(
        out_grad,
        saves[slot_expert],
        full_gate[slot_expert],
        full_up[slot_expert],
        full_down[slot_expert],
    )
    grads_in = slot_grad.reshape(groups, 1, capacity, width)
    gate_g, up_g, down_g = weight_grads(
        inputs[slot_expert], out_grad, gate_term, up_term, saves[slot_expert][3]
    )
    gate_list = [gate_g]
    up_list = [up_g]
    down_list = [down_g]
    slot_grads = grads_in.reshape(experts, capacity, width)
    gate_grad = jnp.stack(gate_list)
    up_grad = jnp.stack(up_list)
    down_grad = jnp.stack(down_list)
    back_grad = lax.all_to_all(slot_grads, "expert", split_axis=0, concat_axis=0, tiled=True)
    out_slots = jnp.dot(
        table, back_out.reshape(experts * capacity, width), preferred_element_type=jnp.float32
    )
    out_slots = out_slots.reshape(count, top, width)
    layer_out = jnp.sum(route_weights[:, :, None] * out_slots, axis=1).astype(jnp.bfloat16)
    route_grad = jnp.sum(grad_out.astype(jnp.float32)[:, None, :] * out_slots, axis=2)
    grad_slots = jnp.dot(
        table, back_grad.reshape(experts * capacity, width), preferred_element_type=jnp.float32
    )
    token_grad = jnp.sum(grad_slots.reshape(count, top, width), axis=1).astype(jnp.bfloat16)
    return (layer_out, token_grad, route_grad, gate_grad, up_grad, down_grad)


def pad16(n):
    return (n + 15) // 16 * 16


def route_tables(ids, weights, groups, chip):
    top, count = ids.shape
    stages = groups // CORES
    lanes = lax.broadcasted_iota(jnp.int32, (1, count), 1).astype(F32)
    experts = lax.broadcasted_iota(jnp.int32, (groups, count), 0)
    hits = [(ids[k:k + 1, :] == experts).astype(F32) for k in range(top)]
    member = sum(hits)
    weight = sum(hit * weights[k:k + 1, :] for k, hit in enumerate(hits))
    first_up = sum(member[groups - CORES + i:groups - CORES + i + 1] for i in range(CORES))
    first_down = sum(member[i:i + 1] for i in range(CORES))
    first = [(f > 0).astype(F32) for f in (first_up, first_down)]
    before = (
        lax.broadcasted_iota(jnp.int32, (count, count), 0) < lax.broadcasted_iota(jnp.int32, (count, count), 1)
    ).astype(BF16)
    counts = jnp.dot(jnp.concatenate([member] + first + [jnp.zeros((groups - 2, count), F32)], axis=0).astype(BF16),
                     before, preferred_element_type=F32)
    slot = jnp.where(member > 0, counts[:groups], -1.0)

    def position(i):
        ahead = counts[groups + i:groups + i + 1]
        number = jnp.sum(first[i], axis=1, keepdims=True)
        return jnp.where(first[i] > 0, ahead, number + lanes - ahead)

    hots = [one_hot(position(i), count) for i in range(2)]
    dest = lax.broadcasted_iota(jnp.int32, (groups, count), 0) // CORES

    def in_order(values, precision):
        up, down = [
            lax.dot_general(values, hot.astype(values.dtype), (((1,), (1,)), ((), ())),
                            precision=precision, preferred_element_type=F32)
            for hot in hots
        ]
        return jnp.where(dest >= chip, up, down)

    slot_rows = in_order(slot.astype(BF16), None)
    weight_rows = in_order(weight, lax.Precision.HIGHEST)
    tiles = []
    for e in range(groups):
        other = e // CORES * CORES + (CORES - 1 - e % CORES)
        row = lambda a, i: a[i:i + 1]
        tiles.append(jnp.concatenate(
            [row(slot_rows, e), row(weight_rows, e), row(slot_rows, other), row(slot, e), row(slot, other),
             jnp.zeros((3, count), F32)], axis=0))
    return tiles, hots[0].astype(BF16), hots[1].astype(BF16), hits


def one_hot(row, height):
    rows = lax.broadcasted_iota(jnp.int32, (height, row.shape[1]), 0).astype(F32)
    return (rows == row).astype(F32)


def choose(index, values):
    result = jnp.int32(values[0])
    for i in range(1, len(values)):
        result = jnp.where(index == i, jnp.int32(values[i]), result)
    return result


def visit_order(chip, stages):
    inner = -1 if 2 * chip >= stages else 1
    near = [s for d in range(stages) for s in ((chip + d * inner, chip - d * inner) if d else (chip,))]
    return [s for s in near if 0 <= s < stages]


def moe_kernel(
    groups, ndp, cap, edge,
    tok_hbm, grad_hbm, ids_ref, weight_ref, wg_hbm, wu_hbm, wd_hbm,
    out_ref, tgrad_ref, route_ref, gg_ref, ug_ref, dg_ref,
    tok, grad, meta_own, blocks, own_down, metas, xr, gr, wr, wgu, wd, yy, ym, ret_in, ret_down, ret_out,
    fa, fb, hid, hs, both, dots, gs, gs2, grx, keep, own, route_out, route_in,
    in_send, in_recv, meta_send, meta_recv, w_send, w_recv, pc_send, pc_recv,
    ret_send, ret_recv, retd_recv, route_send, route_recv, gr_send, gr_recv, load_sem,
):
    stages = groups // CORES
    count, width = tok.shape
    part, ff = gg_ref.shape
    half, hp = count // 2, part // 2
    me = lax.axis_index("expert")
    dp = lax.axis_index("dp")
    chip, core = me // CORES, me % CORES
    mate = chip * CORES + (1 - core)
    px, py = dp % 2, dp // 2
    xn, yn, dg = py * 2 + (1 - px), (1 - py) * 2 + px, (1 - py) * 2 + (1 - px)
    to_mate, to_x, to_y = {"expert": mate}, {"dp": xn}, {"dp": yn}
    at_edge = (chip == 0) | (chip == stages - 1)
    inside = jnp.logical_not(at_edge)
    has_up, has_down = chip < stages - 1, chip > 0
    up_dev, down_dev = {"expert": me + CORES}, {"expert": me - CORES}
    low = 2 * chip < stages
    yes = chip >= 0
    pending = []

    def copy(src, dst, ssem, rsem, where):
        return pltpu.make_async_remote_copy(
            src_ref=src, dst_ref=dst, send_sem=ssem, recv_sem=rsem,
            device_id=where, device_id_type=pl.DeviceIdType.MESH,
        )

    def send(cond, *args):
        if cond is None:
            copy(*args).start()
        else:
            pl.when(cond)(lambda: copy(*args).start())
        pending.append((cond, args))

    def landed(ref, sem):
        copy(ref, ref, sem, sem, to_mate).wait_recv()

    def rows_of(c, short):
        end = half if c == 0 else (edge if short else count)
        return pl.ds(c * half, end - c * half)

    def send_rows(cond, short, c, src, dst, ssem, rsem, where):
        if c == 0 or edge == count:
            send(cond, src.at[rows_of(c, False)], dst.at[rows_of(c, False)], ssem, rsem, where)
            return
        full = jnp.logical_not(short)
        if cond is not None:
            short, full = cond & short, cond & full
        for when, cut in ((full, rows_of(c, False)), (short, rows_of(c, True))):
            send(when, src.at[cut], dst.at[cut], ssem, rsem, where)

    def wait_rows(cond, short, c, dst, sem):
        if c == 0 or edge == count:
            pl.when(cond)(lambda: landed(dst.at[rows_of(c, False)], sem))
            return
        pl.when(cond & jnp.logical_not(short))(lambda: landed(dst.at[rows_of(c, False)], sem))
        pl.when(cond & short)(lambda: landed(dst.at[rows_of(c, True)], sem))

    def nt(a, b):
        return lax.dot_general(a, b, (((1,), (1,)), ((), ())), preferred_element_type=F32)

    def tn(a, b):
        return lax.dot_general(a, b, (((0,), (0,)), ((), ())), preferred_element_type=F32)

    def nn(a, b):
        return jnp.dot(a, b, preferred_element_type=F32)

    gate_cols, up_cols = pl.ds(0, ff), pl.ds(ff, ff)

    def weight(i, j):
        return wd.at[j] if i == 2 else wgu.at[j, :, gate_cols if i == 0 else up_cols]

    loads = [
        pltpu.make_async_copy(src, dst, load_sem.at[n])
        for n, (src, dst) in enumerate((
            (tok_hbm, tok), (wg_hbm, weight(0, dp)), (wu_hbm, weight(1, dp)), (grad_hbm, grad),
            (wd_hbm, weight(2, dp)),
        ))
    ]
    for load in loads:
        load.start()

    barrier = pltpu.get_barrier_semaphore()
    for off in range(1, groups):
        pl.semaphore_signal(barrier, inc=1, device_id={"expert": (me + off) % groups},
                            device_id_type=pl.DeviceIdType.MESH)
    for off in range(1, ndp):
        pl.semaphore_signal(barrier, inc=1, device_id={"dp": (dp + off) % ndp},
                            device_id_type=pl.DeviceIdType.MESH)

    tiles, up_hot, down_hot, hits = route_tables(ids_ref[...], weight_ref[...], groups, chip)
    for e in range(groups):
        meta_own[e] = tiles[e]

    def arrange(t):
        value = (tok, grad)[t][...]
        blocks[0, t, chip] = nn(up_hot, value).astype(BF16)
        own_down[t] = nn(down_hot, value).astype(BF16)

    loads[0].wait()
    arrange(0)
    pl.semaphore_wait(barrier, groups + ndp - 2)

    def depart_up(t, cond, chunks=(0, 1)):
        for c in chunks:
            send_rows(cond, chip + 1 == stages - 1, c, blocks.at[0, t, chip], blocks.at[0, t, chip],
                      in_send.at[t, 0, 0, c], in_recv.at[0, t, chip, c], up_dev)

    def depart_down(t, cond, chunks=(0, 1)):
        for c in chunks:
            send_rows(cond, chip - 1 == 0, c, own_down.at[t], blocks.at[0, t, chip],
                      in_send.at[t, 0, 1, c], in_recv.at[0, t, chip, c], down_dev)

    def depart_mate(t):
        send(None, blocks.at[0, t, chip], blocks.at[1, t, chip],
             in_send.at[t, 0, 2, 0], in_recv.at[1, t, chip, 0], to_mate)

    halves = (pl.ds(0, hp), pl.ds(hp, hp))

    def weight_direct(i):
        for n, (h, where) in enumerate(((0, to_x), (1, to_y), (1, to_x), (0, to_y))):
            ref = weight(i, dp).at[halves[h]]
            send(None, ref, ref, w_send.at[i, n], w_recv.at[i, n], where)

    def weight_relay(i):
        for n, (h, j, where) in enumerate(((0, xn, to_y), (1, yn, to_x))):
            ref = weight(i, j).at[halves[h]]
            landed(ref, w_recv.at[i, n])
            send(None, ref, ref, w_send.at[i, 4 + n], w_recv.at[i, 4 + n], where)

    def weight_rest(i):
        for n, (h, j) in ((2, (1, xn)), (3, (0, yn)), (4, (0, dg)), (5, (1, dg))):
            landed(weight(i, j).at[halves[h]], w_recv.at[i, n])

    depart_up(0, has_up)
    depart_down(0, has_down)
    depart_mate(0)
    for off in range(1, groups):
        other = (me + off) % groups
        send(None, meta_own.at[other], metas.at[me], meta_send.at[off - 1], meta_recv.at[off - 1],
             {"expert": other})
    for i in range(2):
        loads[1 + i].wait()
        weight_direct(i)
    metas[me] = meta_own[me]
    if edge < count:
        rest = pl.ds(edge, count - edge)
        empty = jnp.zeros((count - edge, width), BF16)
        for s in range(stages):
            ends_at = jnp.where(s > chip, chip - 1, chip + 1)
            from_edge = (s != chip) & inside & ((ends_at == 0) | (ends_at == stages - 1))

            @pl.when(at_edge & (s != chip))
            def _():
                for t in range(2):
                    blocks[0, t, s, rest] = empty
                    blocks[1, t, s, rest] = empty

            @pl.when(from_edge | ((s == chip) & (chip + 1 == stages - 1)))
            def _():
                for t in range(2):
                    ret_in[t, s, rest] = empty

        @pl.when(chip - 1 == 0)
        def _():
            for t in range(2):
                ret_down[t, rest] = empty
    for t in range(2):
        @pl.when(chip == stages - 1)
        def _():
            ret_in[t, chip] = jnp.zeros((count, width), BF16)

        @pl.when(chip == 0)
        def _():
            ret_down[t] = jnp.zeros((count, width), BF16)

    loads[3].wait()
    arrange(1)
    depart_up(1, has_up & at_edge)
    depart_down(1, has_down & at_edge)
    depart_mate(1)
    for off in range(1, groups):
        copy(meta_own.at[0], metas.at[0], meta_send.at[off - 1], meta_recv.at[off - 1],
             to_mate).wait_recv()

    table = [visit_order(z, stages) for z in range(stages)]
    source = [choose(chip, [table[z][q] for z in range(stages)]) for q in range(stages)]

    def arrive(t, q, c, role=yes):
        s = source[q]
        nxt = jnp.where(s < chip, chip + 1, chip - 1)
        more = (nxt >= 0) & (nxt < stages)
        wait_rows(role, at_edge, c, blocks.at[0, t, s], in_recv.at[0, t, s, c])
        send_rows(more & role, (nxt == 0) | (nxt == stages - 1), c, blocks.at[0, t, s],
                  blocks.at[0, t, s], in_send.at[t, q, 0, c], in_recv.at[0, t, s, c],
                  {"expert": nxt * CORES + core})
        send_rows(role, at_edge, c, blocks.at[0, t, s], blocks.at[1, t, s],
                  in_send.at[t, q, 2, c], in_recv.at[1, t, s, c], to_mate)

    def compact(t, q):
        s = source[q]
        for r in range(2):
            if r == 1 and q == 0:
                landed(blocks.at[1, t, s], in_recv.at[1, t, s, 0])
            elif r == 1:
                for c in range(2):
                    wait_rows(yes, at_edge, c, blocks.at[1, t, s], in_recv.at[1, t, s, c])
            tile = metas[s * CORES + (core if r == 0 else 1 - core)]
            hot = one_hot(tile[0:1, :], cap)
            rows = pl.ds((q * 2 + r) * cap, cap)
            (xr, gr)[t][rows, :] = nn(hot.astype(BF16), blocks[r, t, s]).astype(BF16)
            if t == 0:
                scale = jnp.sum(hot * tile[1:2, :], axis=1, keepdims=True)
                wr[rows, :] = jnp.broadcast_to(scale, (cap, 128))

    compact(0, 0)
    near = range(1, stages - 1)
    last = stages - 1
    for q in near:
        arrive(0, q, 0)
    for i in range(2):
        weight_relay(i)
    loads[4].wait()
    weight_direct(2)
    for q in near:
        arrive(0, q, 1)
    for q in near:
        compact(0, q)
    high = jnp.logical_not(low)
    depart_up(1, inside & high, (1,))
    depart_down(1, inside & low, (1,))
    arrive(0, last, 0)
    depart_up(1, inside & low)
    depart_down(1, inside & high)
    arrive(0, last, 1)
    depart_up(1, inside & high, (0,))
    depart_down(1, inside & low, (0,))
    compact(0, last)
    for i in range(2):
        weight_rest(i)

    def cut(j):
        return pl.ds(j * part, part)

    def cut_at(j):
        return pl.ds(pl.multiple_of(j * part, part), part)

    total = xr.shape[0]
    gu = jnp.zeros((total, 2 * ff), F32)
    for j in range(ndp):
        gu += nn(xr[:, cut(j)], wgu[j])
    gate, up = gu[:, :ff], gu[:, ff:]
    sig = jax.nn.sigmoid(gate)
    scale = wr[:, 0:1]
    gated = gate * sig
    value = gated * up
    hid[...] = value.astype(BF16)
    hs[...] = (scale * value).astype(BF16)
    fa[...] = scale * (up * sig * (1.0 + gate * (1.0 - sig)))
    fb[...] = scale * gated

    arrive(1, 1, 0)
    for q in near[1:]:
        arrive(1, q, 0, inside)
    weight_relay(2)
    arrive(1, 1, 1)
    for q in near[1:]:
        arrive(1, q, 1, inside)

    def place(t, cols, value, qs):
        for n, q in enumerate(qs):
            yy[t, q, 0:cap, cols] = value[2 * n * cap:(2 * n + 1) * cap]
            ym[t, q, :, cols] = value[(2 * n + 1) * cap:(2 * n + 2) * cap]

    def pair(t, qs):
        for q in reversed(qs):
            send(None, ym.at[t, q], yy.at[t, q, pl.ds(cap, cap)], pc_send.at[t, q],
                 pc_recv.at[t, q], to_mate)

    everyone = range(stages)
    for n, j in enumerate((dp, xn, yn, dg)):
        if n == 1:
            weight_rest(2)
        place(0, cut_at(j), nt(hs[...], wd[j]).astype(BF16), everyone)
    pair(0, everyone)

    def expand(t, q, c, row_own, row_mate):
        tile = metas[source[q] * CORES + core]
        hot = jnp.concatenate(
            [one_hot(tile[row_own:row_own + 1, :], cap), one_hot(tile[row_mate:row_mate + 1, :], cap)],
            axis=0).astype(BF16)
        if c is not None:
            hot = hot[:, c * half:(c + 1) * half]
        return tn(hot, yy[t, q])

    def give_back(t, q, ends):
        s = source[q]
        rising = s > chip
        nxt = jnp.where(rising, chip + 1, chip - 1)
        back = jnp.where(rising, chip - 1, chip + 1)
        where = {"expert": nxt * CORES + core}
        here = at_edge if ends else inside
        arrives = rising & (nxt == s)
        pl.when(here)(lambda: landed(yy.at[t, q, pl.ds(cap, cap)], pc_recv.at[t, q]))
        for c in range(2):
            lines = pl.ds(c * half, half)
            if not ends:
                wait_rows(here, (back == 0) | (back == stages - 1), c, ret_in.at[t, s],
                          ret_recv.at[t, s, c])

            @pl.when(here)
            def _():
                value = expand(t, q, c, 0, 2)
                if not ends:
                    value = value + ret_in[t, s, lines].astype(F32)
                ret_out[t, q, lines] = value.astype(BF16)

            rows = rows_of(c, ends)
            send(here & arrives, ret_out.at[t, q, rows], ret_down.at[t, rows], ret_send.at[t, q, c],
                 retd_recv.at[t, c], where)
            send(here & jnp.logical_not(arrives), ret_out.at[t, q, rows], ret_in.at[t, s, rows],
                 ret_send.at[t, q, c], ret_recv.at[t, s, c], where)

    def backward_hidden(qs):
        rows = pl.ds(qs[0] * 2 * cap, len(qs) * 2 * cap)
        hg = nn(gr[rows, cut(0)], wd[0])
        for j in range(1, ndp):
            hg += nn(gr[rows, cut(j)], wd[j])
        both[rows, :ff] = (hg * fa[rows, :]).astype(BF16)
        both[rows, ff:] = (hg * fb[rows, :]).astype(BF16)
        line = jnp.sum(hg * hid[rows, :].astype(F32), axis=1, keepdims=True)
        dots[rows, :] = jnp.broadcast_to(line, (line.shape[0], 128))

    def backward_rows(qs):
        rows = pl.ds(qs[0] * 2 * cap, len(qs) * 2 * cap)
        for j in range(ndp):
            place(1, cut(j), nt(both[rows, :], wgu[j]).astype(BF16), qs)
        pair(1, qs)

    give_back(0, last, True)
    for q in reversed(near):
        if q > 1:
            give_back(0, q, True)
    arrive(1, last, 0, inside)
    compact(1, 0)
    compact(1, 1)
    for q in near[1:]:
        for c in range(2):
            arrive(1, q, c, at_edge)
        compact(1, q)
    backward_hidden(range(last))
    arrive(1, last, 1, inside)
    backward_rows(range(last))
    for c in range(2):
        arrive(1, last, c, at_edge)
    compact(1, last)
    backward_hidden(range(last, stages))

    def weight_slice(j):
        cols = cut_at(j)
        return nn_t(xr, cols, both), nn_t(gr, cols, hs)

    def nn_t(rows_ref, cols, ref):
        return tn(rows_ref[:, cols], ref[...])

    def pieces(value, down, h):
        top = slice(h * hp, (h + 1) * hp)
        return value[top, :ff], value[top, ff:], down[top]

    def give_grad(k, h, values, where):
        for i, v in enumerate(pieces(*values, h)):
            gs[i, k] = v.astype(BF16)
        for i in range(3):
            send(None, gs.at[i, k], grx.at[i, k], gr_send.at[i, k], gr_recv.at[i, k], where)

    def keep_grad(k, h, values):
        for i, v in enumerate(pieces(*values, h)):
            keep[i, k] = v

    values = weight_slice(dg)
    give_grad(0, 0, values, to_x)
    give_grad(1, 1, values, to_y)
    backward_rows(range(last, stages))
    give_back(0, last, False)
    values = weight_slice(xn)
    give_grad(2, 0, values, to_x)
    keep_grad(1, 1, values)
    give_back(1, last, True)
    values = weight_slice(yn)
    give_grad(3, 1, values, to_y)
    keep_grad(0, 0, values)
    for q in near:
        give_back(0, q, False)
    for q in reversed(near):
        if q > 1:
            give_back(1, q, True)
    for t in range(2):
        give_back(t, 1, True)

    for q in range(stages):
        for r in range(2):
            origin = source[q] * CORES + (core if r == 0 else 1 - core)
            hot = one_hot(metas[origin][3:4, :], cap)
            part_dots = dots[(q * 2 + r) * cap:(q * 2 + r + 1) * cap, 0:1]
            line = jnp.sum(hot * part_dots, axis=0, keepdims=True)
            route_out[origin] = jnp.broadcast_to(line, (8, count))
    for off in range(1, groups):
        other = (me + off) % groups
        send(None, route_out.at[other], route_in.at[me], route_send.at[off - 1],
             route_recv.at[off - 1], {"expert": other})
    route_in[me] = route_out[me]

    values = weight_slice(dp)
    for h in range(2):
        for i, v in enumerate(pieces(*values, h)):
            own[i, h] = v

    give_back(1, last, False)
    for i in range(3):
        for k, where in ((0, to_y), (1, to_x)):
            landed(grx.at[i, k], gr_recv.at[i, k])
            gs2[i, k] = (keep[i, k] + grx[i, k].astype(F32)).astype(BF16)
            send(None, gs2.at[i, k], grx.at[i, 4 + k], gr_send.at[i, 4 + k], gr_recv.at[i, 4 + k],
                 where)
    for q in near:
        give_back(1, q, False)

    for t, ref in enumerate((out_ref, tgrad_ref)):
        landed(yy.at[t, 0, pl.ds(cap, cap)], pc_recv.at[t, 0])
        value = expand(t, 0, None, 3, 4)
        for c in range(2):
            wait_rows(has_up, chip + 1 == stages - 1, c, ret_in.at[t, chip], ret_recv.at[t, chip, c])
            wait_rows(has_down, chip - 1 == 0, c, ret_down.at[t], retd_recv.at[t, c])
        value += tn(up_hot, ret_in[t, chip]) + tn(down_hot, ret_down[t])
        ref[...] = value.astype(BF16)

    for off in range(1, groups):
        copy(route_out.at[0], route_in.at[0], route_send.at[off - 1], route_recv.at[off - 1],
             to_mate).wait_recv()
    for k, hit in enumerate(hits):
        line = sum(hit[e:e + 1] * route_in[e, 0:1] for e in range(groups))
        route_ref[k:k + 1, :] = line
    for i, ref in enumerate((gg_ref, ug_ref, dg_ref)):
        for h in range(2):
            value = own[i, h]
            for k in (2 + h, 4 + h):
                landed(grx.at[i, k], gr_recv.at[i, k])
                value += grx[i, k].astype(F32)
            ref[halves[h]] = value.astype(BF16)
    for cond, args in pending:
        if cond is None:
            copy(*args).wait_send()
        else:
            pl.when(cond)(lambda args=args: copy(*args).wait_send())


def flush_kernel(*refs):
    number = (len(refs) - 1) // 2
    copies = [
        pltpu.make_async_copy(refs[n], refs[number + n], refs[-1].at[n]) for n in range(number)
    ]
    for cp in copies:
        cp.start()
    for cp in copies:
        cp.wait()


def flush(*arrays):
    return pl.pallas_call(
        flush_kernel,
        out_shape=tuple(jax.ShapeDtypeStruct(a.shape, a.dtype) for a in arrays),
        in_specs=[pl.BlockSpec(memory_space=pltpu.VMEM)] * len(arrays),
        out_specs=(pl.BlockSpec(memory_space=pltpu.HBM),) * len(arrays),
        scratch_shapes=[pltpu.SemaphoreType.DMA((len(arrays),))],
    )(*(pltpu.with_memory_space_constraint(a, pltpu.VMEM) for a in arrays))


def kernel_scratch(groups, ndp, cap, count, width, part, ff):
    stages = groups // CORES
    rows = groups * cap
    hp = part // 2
    shapes = [
        ((count, width), BF16),
        ((count, width), BF16),
        ((groups, 8, count), F32),
        ((2, 2, stages, count, width), BF16),
        ((2, count, width), BF16),
        ((groups, 8, count), F32),
        ((rows, width), BF16),
        ((rows, width), BF16),
        ((rows, 128), F32),
        ((ndp, part, 2 * ff), BF16),
        ((ndp, part, ff), BF16),
        ((2, stages, 2 * cap, width), BF16),
        ((2, stages, cap, width), BF16),
        ((2, stages, count, width), BF16),
        ((2, count, width), BF16),
        ((2, stages, count, width), BF16),
        ((rows, ff), F32),
        ((rows, ff), F32),
        ((rows, ff), BF16),
        ((rows, ff), BF16),
        ((rows, 2 * ff), BF16),
        ((rows, 128), F32),
        ((3, 4, hp, ff), BF16),
        ((3, 2, hp, ff), BF16),
        ((3, 6, hp, ff), BF16),
        ((3, 2, hp, ff), F32),
        ((3, 2, hp, ff), F32),
        ((groups, 8, count), F32),
        ((groups, 8, count), F32),
    ]
    sems = [
        (2, stages, 3, 2), (2, 2, stages, 2), (groups - 1,), (groups - 1,), (3, 6), (3, 6),
        (2, stages), (2, stages), (2, stages, 2), (2, stages, 2), (2, 2), (groups - 1,),
        (groups - 1,), (3, 6), (3, 6), (5,),
    ]
    return shapes, sems


def scratch_bytes(shapes):
    total = 0
    for shape, dtype in shapes:
        size = jnp.dtype(dtype).itemsize
        for n in shape:
            size *= n
        total += size
    return total


def slot_capacity(count, top, experts):
    return max(2, (3 * count * top + 2 * experts - 1) // (2 * experts))


def line_body(groups, ndp, tokens, expert_ids, route_weights, w_gate, w_up, w_down, grad_out):
    count, width = tokens.shape
    _, part, ff = w_gate.shape
    top = expert_ids.shape[1]
    slots = slot_capacity(count, top, groups)
    cap = pad16(slots)
    edge = min(count, pad16(CORES * slots))
    shapes, sems = kernel_scratch(groups, ndp, cap, count, width, part, ff)
    vmem = pl.BlockSpec(memory_space=pltpu.VMEM)
    hbm = pl.BlockSpec(memory_space=pltpu.HBM)
    outs = pl.pallas_call(
        functools.partial(moe_kernel, groups, ndp, cap, edge),
        out_shape=(
            pltpu.VMEM((count, width), BF16),
            pltpu.VMEM((count, width), BF16),
            pltpu.VMEM((top, count), F32),
            pltpu.VMEM((part, ff), BF16),
            pltpu.VMEM((part, ff), BF16),
            pltpu.VMEM((part, ff), BF16),
        ),
        in_specs=[hbm, hbm, vmem, vmem, hbm, hbm, hbm],
        out_specs=(vmem,) * 6,
        scratch_shapes=[pltpu.VMEM(s, d) for s, d in shapes]
        + [pltpu.SemaphoreType.DMA(s) for s in sems],
        compiler_params=pltpu.CompilerParams(
            collective_id=0, has_side_effects=True, vmem_limit_bytes=VMEM_MAX
        ),
    )(tokens, grad_out, expert_ids.T, route_weights.T, w_gate[0], w_up[0], w_down[0])
    layer_out, token_grad, route, gate_g, up_g, down_g = flush(*outs)
    return layer_out, token_grad, route.T, gate_g[None], up_g[None], down_g[None]


def pick_body(groups, ndp, *args):
    tokens, expert_ids, _, w_gate = args[:4]
    count, width = tokens.shape
    local, part, ff = w_gate.shape
    if local == 1 and groups == 4 * CORES and ndp == 4:
        slots = slot_capacity(count, expert_ids.shape[1], groups)
        shapes, _ = kernel_scratch(groups, ndp, pad16(slots), count, width, part, ff)
        tiled = count % 32 == 0 and part % 128 == 0 and ff % 128 == 0 and 4 * slots > count
        if tiled and scratch_bytes(shapes) < VMEM_MAX * 9 // 10:
            return line_body(groups, ndp, *args)
    return body(*args)


def solution(mesh):
    in_specs = (
        P(("dp", "expert"), None),
        P(("dp", "expert"), None),
        P(("dp", "expert"), None),
        P("expert", "dp", None),
        P("expert", "dp", None),
        P("expert", "dp", None),
        P(("dp", "expert"), None),
    )
    out_specs = (
        P(("dp", "expert"), None),
        P(("dp", "expert"), None),
        P(("dp", "expert"), None),
        P("expert", "dp", None),
        P("expert", "dp", None),
        P("expert", "dp", None),
    )
    step = functools.partial(pick_body, mesh.shape["expert"], mesh.shape["dp"])
    return jax.shard_map(step, mesh=mesh, in_specs=in_specs, out_specs=out_specs, check_vma=False)
```

```python
import functools

import jax
import jax.numpy as jnp
from jax import lax
from jax.experimental import pallas as pl
from jax.experimental.pallas import tpu as pltpu
from jax.sharding import PartitionSpec as P

BF16 = jnp.bfloat16
F32 = jnp.float32
CORES = 2
VMEM_MAX = 56 * 1024 * 1024


def slot_table(expert_ids, experts, capacity):
    flat = expert_ids.reshape(-1)
    count = flat.shape[0]
    same = flat[:, None] == flat[None, :]
    earlier = lax.broadcasted_iota(jnp.int32, (count, count), 0) > lax.broadcasted_iota(
        jnp.int32, (count, count), 1
    )
    rank = jnp.sum((same & earlier).astype(jnp.int32), axis=1)
    target = flat * capacity + rank
    columns = lax.broadcasted_iota(jnp.int32, (count, experts * capacity), 1)
    return (target[:, None] == columns).astype(jnp.bfloat16)


def contract_last(left, right):
    return lax.dot_general(
        left, right, (((1,), (1,)), ((), ())), preferred_element_type=jnp.float32
    )


def contract_first(left, right):
    return lax.dot_general(
        left, right, (((0,), (0,)), ((), ())), preferred_element_type=jnp.float32
    )


def expert_forward(rows, gate_w, up_w, down_w):
    gate = jnp.dot(rows, gate_w, preferred_element_type=jnp.float32)
    up = jnp.dot(rows, up_w, preferred_element_type=jnp.float32)
    sig = jax.nn.sigmoid(gate)
    hidden = (gate * sig * up).astype(jnp.bfloat16)
    expert_out = contract_last(hidden, down_w).astype(jnp.bfloat16)
    return (expert_out, (gate, up, sig, hidden))


def expert_backward(out_grad, saved, gate_w, up_w, down_w):
    gate, up, sig, hidden = saved
    hidden_grad = jnp.dot(out_grad, down_w, preferred_element_type=jnp.float32)
    gate_term = (hidden_grad * up * sig * (1.0 + gate * (1.0 - sig))).astype(jnp.bfloat16)
    up_term = (hidden_grad * gate * sig).astype(jnp.bfloat16)
    slot_grad = (contract_last(gate_term, gate_w) + contract_last(up_term, up_w)).astype(
        jnp.bfloat16
    )
    return (slot_grad, gate_term, up_term)


def weight_grads(rows, out_grad, gate_term, up_term, hidden):
    part_rows, part_grad = (
        lax.all_to_all(rows, "dp", split_axis=1, concat_axis=0, tiled=True),
        lax.all_to_all(out_grad, "dp", split_axis=1, concat_axis=0, tiled=True),
    )
    all_gate, all_up, all_hidden = (
        lax.all_gather(gate_term, "dp", axis=0, tiled=True),
        lax.all_gather(up_term, "dp", axis=0, tiled=True),
        lax.all_gather(hidden, "dp", axis=0, tiled=True),
    )
    down_g = contract_first(part_grad, all_hidden).astype(jnp.bfloat16)
    gate_g = contract_first(part_rows, all_gate).astype(jnp.bfloat16)
    up_g = contract_first(part_rows, all_up).astype(jnp.bfloat16)
    return (gate_g, up_g, down_g)


def body(tokens, expert_ids, route_weights, w_gate, w_up, w_down, grad_out):
    local = w_gate.shape[0]
    groups = lax.axis_size("expert")
    experts = local * groups
    count = tokens.shape[0]
    top = expert_ids.shape[1]
    width = tokens.shape[1]
    capacity = max(2, (3 * count * top + 2 * experts - 1) // (2 * experts))
    table = slot_table(expert_ids, experts, capacity)
    per_token = jnp.sum(table.reshape(count, top, experts * capacity), axis=1)
    send_rows = jnp.dot(per_token.T, tokens, preferred_element_type=jnp.float32)
    send_rows = send_rows.astype(jnp.bfloat16).reshape(experts, capacity, width)
    weighted = (route_weights[:, :, None] * grad_out.astype(jnp.float32)[:, None, :]).astype(
        jnp.bfloat16
    )
    send_grad = jnp.dot(
        table.T, weighted.reshape(count * top, width), preferred_element_type=jnp.float32
    )
    send_grad = send_grad.astype(jnp.bfloat16).reshape(experts, capacity, width)
    full_gate, full_up, full_down = (
        lax.all_gather(w_gate, "dp", axis=1, tiled=True),
        lax.all_gather(w_up, "dp", axis=1, tiled=True),
        lax.all_gather(w_down, "dp", axis=1, tiled=True),
    )
    received = lax.all_to_all(send_rows, "expert", split_axis=0, concat_axis=0, tiled=True)
    shaped = received.reshape(groups, local, capacity, width)
    saves = []
    inputs = []
    slot_expert = 0
    rows = shaped[:, slot_expert].reshape(groups * capacity, width)
    expert_out, saved = expert_forward(
        rows, full_gate[slot_expert], full_up[slot_expert], full_down[slot_expert]
    )
    outs = expert_out.reshape(groups, 1, capacity, width)
    saves.append(saved)
    inputs.append(rows)
    expert_outs, saves, inputs = (outs.reshape(experts, capacity, width), saves, inputs)
    back_out = lax.all_to_all(expert_outs, "expert", split_axis=0, concat_axis=0, tiled=True)
    received_grad = lax.all_to_all(send_grad, "expert", split_axis=0, concat_axis=0, tiled=True)
    shaped = received_grad.reshape(groups, local, capacity, width)
    slot_expert = 0
    out_grad = shaped[:, slot_expert].reshape(groups * capacity, width)
    slot_grad, gate_term, up_term = expert_backward(
        out_grad,
        saves[slot_expert],
        full_gate[slot_expert],
        full_up[slot_expert],
        full_down[slot_expert],
    )
    grads_in = slot_grad.reshape(groups, 1, capacity, width)
    gate_g, up_g, down_g = weight_grads(
        inputs[slot_expert], out_grad, gate_term, up_term, saves[slot_expert][3]
    )
    gate_list = [gate_g]
    up_list = [up_g]
    down_list = [down_g]
    slot_grads = grads_in.reshape(experts, capacity, width)
    gate_grad = jnp.stack(gate_list)
    up_grad = jnp.stack(up_list)
    down_grad = jnp.stack(down_list)
    back_grad = lax.all_to_all(slot_grads, "expert", split_axis=0, concat_axis=0, tiled=True)
    out_slots = jnp.dot(
        table, back_out.reshape(experts * capacity, width), preferred_element_type=jnp.float32
    )
    out_slots = out_slots.reshape(count, top, width)
    layer_out = jnp.sum(route_weights[:, :, None] * out_slots, axis=1).astype(jnp.bfloat16)
    route_grad = jnp.sum(grad_out.astype(jnp.float32)[:, None, :] * out_slots, axis=2)
    grad_slots = jnp.dot(
        table, back_grad.reshape(experts * capacity, width), preferred_element_type=jnp.float32
    )
    token_grad = jnp.sum(grad_slots.reshape(count, top, width), axis=1).astype(jnp.bfloat16)
    return (layer_out, token_grad, route_grad, gate_grad, up_grad, down_grad)


def pad16(n):
    return (n + 15) // 16 * 16


def route_tables(ids, weights, groups, chip):
    top, count = ids.shape
    stages = groups // CORES
    lanes = lax.broadcasted_iota(jnp.int32, (1, count), 1).astype(F32)
    experts = lax.broadcasted_iota(jnp.int32, (groups, count), 0)
    hits = [(ids[k:k + 1, :] == experts).astype(F32) for k in range(top)]
    member = sum(hits)
    weight = sum(hit * weights[k:k + 1, :] for k, hit in enumerate(hits))
    first_up = sum(member[groups - CORES + i:groups - CORES + i + 1] for i in range(CORES))
    first_down = sum(member[i:i + 1] for i in range(CORES))
    first = [(f > 0).astype(F32) for f in (first_up, first_down)]
    before = (
        lax.broadcasted_iota(jnp.int32, (count, count), 0) < lax.broadcasted_iota(jnp.int32, (count, count), 1)
    ).astype(BF16)
    counts = jnp.dot(jnp.concatenate([member] + first + [jnp.zeros((groups - 2, count), F32)], axis=0).astype(BF16),
                     before, preferred_element_type=F32)
    slot = jnp.where(member > 0, counts[:groups], -1.0)

    def position(i):
        ahead = counts[groups + i:groups + i + 1]
        number = jnp.sum(first[i], axis=1, keepdims=True)
        return jnp.where(first[i] > 0, ahead, number + lanes - ahead)

    hots = [one_hot(position(i), count) for i in range(2)]
    dest = lax.broadcasted_iota(jnp.int32, (groups, count), 0) // CORES

    def in_order(values, precision):
        up, down = [
            lax.dot_general(values, hot.astype(values.dtype), (((1,), (1,)), ((), ())),
                            precision=precision, preferred_element_type=F32)
            for hot in hots
        ]
        return jnp.where(dest >= chip, up, down)

    slot_rows = in_order(slot.astype(BF16), None)
    weight_rows = in_order(weight, lax.Precision.HIGHEST)
    tiles = []
    for e in range(groups):
        other = e // CORES * CORES + (CORES - 1 - e % CORES)
        row = lambda a, i: a[i:i + 1]
        tiles.append(jnp.concatenate(
            [row(slot_rows, e), row(weight_rows, e), row(slot_rows, other), row(slot, e), row(slot, other),
             jnp.zeros((3, count), F32)], axis=0))
    return tiles, hots[0].astype(BF16), hots[1].astype(BF16), hits


def one_hot(row, height):
    rows = lax.broadcasted_iota(jnp.int32, (height, row.shape[1]), 0).astype(F32)
    return (rows == row).astype(F32)


def choose(index, values):
    result = jnp.int32(values[0])
    for i in range(1, len(values)):
        result = jnp.where(index == i, jnp.int32(values[i]), result)
    return result


def visit_order(chip, stages):
    inner = -1 if 2 * chip >= stages else 1
    near = [s for d in range(stages) for s in ((chip + d * inner, chip - d * inner) if d else (chip,))]
    return [s for s in near if 0 <= s < stages]


def moe_kernel(
    groups, ndp, cap, edge,
    tok_hbm, grad_hbm, ids_ref, weight_ref, wg_hbm, wu_hbm, wd_hbm,
    out_ref, tgrad_ref, route_ref, gg_ref, ug_ref, dg_ref,
    tok, grad, meta_own, blocks, own_down, metas, xr, gr, wr, wgu, wd, yy, ym, ret_in, ret_down, ret_out,
    fa, fb, hid, hs, both, dots, gs, gs2, grx, keep, own, ex, route_out, route_in,
    in_send, in_recv, meta_send, meta_recv, w_send, w_recv, pc_send, pc_recv,
    ret_send, ret_recv, retd_recv, route_send, route_recv, gr_send, gr_recv, load_sem,
):
    stages = groups // CORES
    count, width = tok.shape
    part, ff = gg_ref.shape
    half, hp = count // 2, part // 2
    me = lax.axis_index("expert")
    dp = lax.axis_index("dp")
    chip, core = me // CORES, me % CORES
    mate = chip * CORES + (1 - core)
    px, py = dp % 2, dp // 2
    xn, yn, dg = py * 2 + (1 - px), (1 - py) * 2 + px, (1 - py) * 2 + (1 - px)
    to_mate, to_x, to_y = {"expert": mate}, {"dp": xn}, {"dp": yn}
    at_edge = (chip == 0) | (chip == stages - 1)
    inside = jnp.logical_not(at_edge)
    has_up, has_down = chip < stages - 1, chip > 0
    up_dev, down_dev = {"expert": me + CORES}, {"expert": me - CORES}
    low = 2 * chip < stages
    yes = chip >= 0
    pending = []

    def copy(src, dst, ssem, rsem, where):
        return pltpu.make_async_remote_copy(
            src_ref=src, dst_ref=dst, send_sem=ssem, recv_sem=rsem,
            device_id=where, device_id_type=pl.DeviceIdType.MESH,
        )

    def send(cond, *args):
        if cond is None:
            copy(*args).start()
        else:
            pl.when(cond)(lambda: copy(*args).start())
        pending.append((cond, args))

    def landed(ref, sem):
        copy(ref, ref, sem, sem, to_mate).wait_recv()

    def rows_of(c, short):
        end = half if c == 0 else (edge if short else count)
        return pl.ds(c * half, end - c * half)

    def send_rows(cond, short, c, src, dst, ssem, rsem, where):
        if c == 0 or edge == count:
            send(cond, src.at[rows_of(c, False)], dst.at[rows_of(c, False)], ssem, rsem, where)
            return
        full = jnp.logical_not(short)
        if cond is not None:
            short, full = cond & short, cond & full
        for when, cut in ((full, rows_of(c, False)), (short, rows_of(c, True))):
            send(when, src.at[cut], dst.at[cut], ssem, rsem, where)

    def wait_rows(cond, short, c, dst, sem):
        if c == 0 or edge == count:
            pl.when(cond)(lambda: landed(dst.at[rows_of(c, False)], sem))
            return
        pl.when(cond & jnp.logical_not(short))(lambda: landed(dst.at[rows_of(c, False)], sem))
        pl.when(cond & short)(lambda: landed(dst.at[rows_of(c, True)], sem))

    def nt(a, b):
        return lax.dot_general(a, b, (((1,), (1,)), ((), ())), preferred_element_type=F32)

    def tn(a, b):
        return lax.dot_general(a, b, (((0,), (0,)), ((), ())), preferred_element_type=F32)

    def nn(a, b):
        return jnp.dot(a, b, preferred_element_type=F32)

    gate_cols, up_cols = pl.ds(0, ff), pl.ds(ff, ff)

    def weight(i, j):
        return wd.at[j] if i == 2 else wgu.at[j, :, gate_cols if i == 0 else up_cols]

    loads = [
        pltpu.make_async_copy(src, dst, load_sem.at[n])
        for n, (src, dst) in enumerate((
            (tok_hbm, tok), (wg_hbm, weight(0, dp)), (wu_hbm, weight(1, dp)), (grad_hbm, grad),
            (wd_hbm, weight(2, dp)),
        ))
    ]
    for load in loads:
        load.start()

    barrier = pltpu.get_barrier_semaphore()
    for off in range(1, groups):
        pl.semaphore_signal(barrier, inc=1, device_id={"expert": (me + off) % groups},
                            device_id_type=pl.DeviceIdType.MESH)
    for off in range(1, ndp):
        pl.semaphore_signal(barrier, inc=1, device_id={"dp": (dp + off) % ndp},
                            device_id_type=pl.DeviceIdType.MESH)

    tiles, up_hot, down_hot, hits = route_tables(ids_ref[...], weight_ref[...], groups, chip)
    for e in range(groups):
        meta_own[e] = tiles[e]

    def arrange(t):
        value = (tok, grad)[t][...]
        blocks[0, t, chip] = nn(up_hot, value).astype(BF16)
        own_down[t] = nn(down_hot, value).astype(BF16)

    loads[0].wait()
    arrange(0)
    pl.semaphore_wait(barrier, groups + ndp - 2)

    def depart_up(t, cond, chunks=(0, 1)):
        for c in chunks:
            send_rows(cond, chip + 1 == stages - 1, c, blocks.at[0, t, chip], blocks.at[0, t, chip],
                      in_send.at[t, 0, 0, c], in_recv.at[0, t, chip, c], up_dev)

    def depart_down(t, cond, chunks=(0, 1)):
        for c in chunks:
            send_rows(cond, chip - 1 == 0, c, own_down.at[t], blocks.at[0, t, chip],
                      in_send.at[t, 0, 1, c], in_recv.at[0, t, chip, c], down_dev)

    def depart_mate(t):
        send(None, blocks.at[0, t, chip], blocks.at[1, t, chip],
             in_send.at[t, 0, 2, 0], in_recv.at[1, t, chip, 0], to_mate)

    halves = (pl.ds(0, hp), pl.ds(hp, hp))

    def weight_direct(i):
        for n, (h, where) in enumerate(((0, to_x), (1, to_y), (1, to_x), (0, to_y))):
            ref = weight(i, dp).at[halves[h]]
            send(None, ref, ref, w_send.at[i, n], w_recv.at[i, n], where)

    def weight_relay(i):
        for n, (h, j, where) in enumerate(((0, xn, to_y), (1, yn, to_x))):
            ref = weight(i, j).at[halves[h]]
            landed(ref, w_recv.at[i, n])
            send(None, ref, ref, w_send.at[i, 4 + n], w_recv.at[i, 4 + n], where)

    def weight_rest(i, ns=range(2, 6)):
        for n in ns:
            h, j = ((1, xn), (0, yn), (0, dg), (1, dg))[n - 2]
            landed(weight(i, j).at[halves[h]], w_recv.at[i, n])

    depart_up(0, has_up)
    depart_down(0, has_down)
    depart_mate(0)
    for off in range(1, groups):
        other = (me + off) % groups
        send(None, meta_own.at[other], metas.at[me], meta_send.at[off - 1], meta_recv.at[off - 1],
             {"expert": other})
    for i in range(2):
        loads[1 + i].wait()
        weight_direct(i)
    metas[me] = meta_own[me]
    if edge < count:
        rest = pl.ds(edge, count - edge)
        empty = jnp.zeros((count - edge, width), BF16)
        for s in range(stages):
            ends_at = jnp.where(s > chip, chip - 1, chip + 1)
            from_edge = (s != chip) & inside & ((ends_at == 0) | (ends_at == stages - 1))

            @pl.when(at_edge & (s != chip))
            def _():
                for t in range(2):
                    blocks[0, t, s, rest] = empty
                    blocks[1, t, s, rest] = empty

            @pl.when(from_edge | ((s == chip) & (chip + 1 == stages - 1)))
            def _():
                for t in range(2):
                    ret_in[t, s, rest] = empty

        @pl.when(chip - 1 == 0)
        def _():
            for t in range(2):
                ret_down[t, rest] = empty
    for t in range(2):
        @pl.when(chip == stages - 1)
        def _():
            ret_in[t, chip] = jnp.zeros((count, width), BF16)

        @pl.when(chip == 0)
        def _():
            ret_down[t] = jnp.zeros((count, width), BF16)

    loads[3].wait()
    arrange(1)
    depart_up(1, has_up & at_edge)
    depart_down(1, has_down & at_edge)
    depart_mate(1)
    for off in range(1, groups):
        copy(meta_own.at[0], metas.at[0], meta_send.at[off - 1], meta_recv.at[off - 1],
             to_mate).wait_recv()

    table = [visit_order(z, stages) for z in range(stages)]
    source = [choose(chip, [table[z][q] for z in range(stages)]) for q in range(stages)]

    def arrive(t, q, c, role=yes):
        s = source[q]
        nxt = jnp.where(s < chip, chip + 1, chip - 1)
        more = (nxt >= 0) & (nxt < stages)
        wait_rows(role, at_edge, c, blocks.at[0, t, s], in_recv.at[0, t, s, c])
        send_rows(more & role, (nxt == 0) | (nxt == stages - 1), c, blocks.at[0, t, s],
                  blocks.at[0, t, s], in_send.at[t, q, 0, c], in_recv.at[0, t, s, c],
                  {"expert": nxt * CORES + core})
        send_rows(role, at_edge, c, blocks.at[0, t, s], blocks.at[1, t, s],
                  in_send.at[t, q, 2, c], in_recv.at[1, t, s, c], to_mate)

    def compact(t, q):
        s = source[q]
        for r in range(2):
            if r == 1 and q == 0:
                landed(blocks.at[1, t, s], in_recv.at[1, t, s, 0])
            elif r == 1:
                for c in range(2):
                    wait_rows(yes, at_edge, c, blocks.at[1, t, s], in_recv.at[1, t, s, c])
            tile = metas[s * CORES + (core if r == 0 else 1 - core)]
            hot = one_hot(tile[0:1, :], cap)
            rows = pl.ds((q * 2 + r) * cap, cap)
            (xr, gr)[t][rows, :] = nn(hot.astype(BF16), blocks[r, t, s]).astype(BF16)
            if t == 0:
                scale = jnp.sum(hot * tile[1:2, :], axis=1, keepdims=True)
                wr[rows, :] = jnp.broadcast_to(scale, (cap, 128))

    compact(0, 0)
    near = range(1, stages - 1)
    last = stages - 1
    for q in near:
        arrive(0, q, 0)
    for i in range(2):
        weight_relay(i)
    loads[4].wait()
    weight_direct(2)
    for q in near:
        arrive(0, q, 1)
    for q in near:
        compact(0, q)
    high = jnp.logical_not(low)
    depart_up(1, inside & high, (1,))
    depart_down(1, inside & low, (1,))
    arrive(0, last, 0)
    depart_up(1, inside & low)
    depart_down(1, inside & high)
    arrive(0, last, 1)
    depart_up(1, inside & high, (0,))
    depart_down(1, inside & low, (0,))
    compact(0, last)
    for i in range(2):
        weight_rest(i)

    def cut(j):
        return pl.ds(j * part, part)

    def cut_at(j):
        return pl.ds(pl.multiple_of(j * part, part), part)

    total = xr.shape[0]
    gu = jnp.zeros((total, 2 * ff), F32)
    for j in range(ndp):
        gu += nn(xr[:, cut(j)], wgu[j])
    gate, up = gu[:, :ff], gu[:, ff:]
    sig = jax.nn.sigmoid(gate)
    scale = wr[:, 0:1]
    gated = gate * sig
    value = gated * up
    hid[...] = value.astype(BF16)
    hs[...] = (scale * value).astype(BF16)
    fa[...] = scale * (up * sig * (1.0 + gate * (1.0 - sig)))
    fb[...] = scale * gated

    weight_relay(2)
    arrive(1, 1, 0)
    for q in near[1:]:
        arrive(1, q, 0, inside)
    arrive(1, 1, 1)
    for q in near[1:]:
        arrive(1, q, 1, inside)

    def place(t, cols, value, qs):
        for n, q in enumerate(qs):
            yy[t, q, 0:cap, cols] = value[2 * n * cap:(2 * n + 1) * cap]
            ym[t, q, :, cols] = value[(2 * n + 1) * cap:(2 * n + 2) * cap]

    def pair(t, qs):
        for q in reversed(qs):
            send(None, ym.at[t, q], yy.at[t, q, pl.ds(cap, cap)], pc_send.at[t, q],
                 pc_recv.at[t, q], to_mate)

    everyone = range(stages)
    for n, j in enumerate((dp, xn, yn, dg)):
        if n == 1:
            weight_rest(2, (2, 3))
        if n == 3:
            weight_rest(2, (4, 5))
        place(0, cut_at(j), nt(hs[...], wd[j]).astype(BF16), everyone)
    pair(0, everyone)

    def expand(t, q, row_own, row_mate):
        tile = metas[source[q] * CORES + core]
        hot = jnp.concatenate(
            [one_hot(tile[row_own:row_own + 1, :], cap), one_hot(tile[row_mate:row_mate + 1, :], cap)],
            axis=0).astype(BF16)
        return tn(hot, yy[t, q])

    bounds = (0, half // 2, half, edge, count)
    chunks = [pl.ds(lo, hi - lo) for lo, hi in zip(bounds, bounds[1:])]

    def wait_chunk(cond, short, k, dst, sem):
        if k == len(chunks) - 1:
            cond = cond & jnp.logical_not(short)
        pl.when(cond)(lambda: landed(dst.at[chunks[k]], sem))

    def give_back(t, q, ends):
        s = source[q]
        rising = s > chip
        nxt = jnp.where(rising, chip + 1, chip - 1)
        back = jnp.where(rising, chip - 1, chip + 1)
        where = {"expert": nxt * CORES + core}
        here = at_edge if ends else inside
        arrives = rising & (nxt == s)
        short = (back == 0) | (back == stages - 1)

        @pl.when(here)
        def _():
            landed(yy.at[t, q, pl.ds(cap, cap)], pc_recv.at[t, q])
            ex[...] = expand(t, q, 0, 2)

        for k, rows in enumerate(chunks):
            if ends and k == len(chunks) - 1:
                continue
            if not ends:
                wait_chunk(here, short, k, ret_in.at[t, s], ret_recv.at[t, s, k])

            @pl.when(here)
            def _():
                value = ex[rows]
                if not ends:
                    value = value + ret_in[t, s, rows].astype(F32)
                ret_out[t, q, rows] = value.astype(BF16)

            send(here & arrives, ret_out.at[t, q, rows], ret_down.at[t, rows], ret_send.at[t, q, k],
                 retd_recv.at[t, k], where)
            send(here & jnp.logical_not(arrives), ret_out.at[t, q, rows], ret_in.at[t, s, rows],
                 ret_send.at[t, q, k], ret_recv.at[t, s, k], where)

    def backward_hidden(qs):
        rows = pl.ds(qs[0] * 2 * cap, len(qs) * 2 * cap)
        hg = nn(gr[rows, cut(0)], wd[0])
        for j in range(1, ndp):
            hg += nn(gr[rows, cut(j)], wd[j])
        both[rows, :ff] = (hg * fa[rows, :]).astype(BF16)
        both[rows, ff:] = (hg * fb[rows, :]).astype(BF16)
        line = jnp.sum(hg * hid[rows, :].astype(F32), axis=1, keepdims=True)
        dots[rows, :] = jnp.broadcast_to(line, (line.shape[0], 128))

    def backward_rows(qs):
        rows = pl.ds(qs[0] * 2 * cap, len(qs) * 2 * cap)
        for j in range(ndp):
            place(1, cut(j), nt(both[rows, :], wgu[j]).astype(BF16), qs)
        pair(1, qs)

    give_back(0, last, True)
    for q in reversed(near):
        if q > 1:
            give_back(0, q, True)
    arrive(1, last, 0, inside)
    compact(1, 0)
    compact(1, 1)
    for q in near[1:]:
        for c in range(2):
            arrive(1, q, c, at_edge)
        compact(1, q)
    backward_hidden(range(last))
    arrive(1, last, 1, inside)
    backward_rows(range(last))
    give_back(0, last, False)
    for c in range(2):
        arrive(1, last, c, at_edge)
    compact(1, last)
    backward_hidden(range(last, stages))

    def weight_slice(j):
        cols = cut_at(j)
        return nn_t(xr, cols, both), nn_t(gr, cols, hs)

    def nn_t(rows_ref, cols, ref):
        return tn(rows_ref[:, cols], ref[...])

    def pieces(value, down, h):
        top = slice(h * hp, (h + 1) * hp)
        return value[top, :ff], value[top, ff:], down[top]

    def give_grad(k, h, values, where):
        for i, v in enumerate(pieces(*values, h)):
            gs[i, k] = v.astype(BF16)
        for i in range(3):
            send(None, gs.at[i, k], grx.at[i, k], gr_send.at[i, k], gr_recv.at[i, k], where)

    def keep_grad(k, h, values):
        for i, v in enumerate(pieces(*values, h)):
            keep[i, k] = v

    values = weight_slice(dg)
    give_grad(0, 0, values, to_x)
    give_grad(1, 1, values, to_y)
    backward_rows(range(last, stages))
    values = weight_slice(xn)
    give_grad(2, 0, values, to_x)
    keep_grad(1, 1, values)
    give_back(1, last, True)
    values = weight_slice(yn)
    give_grad(3, 1, values, to_y)
    keep_grad(0, 0, values)
    for q in near:
        give_back(0, q, False)
    for q in reversed(near):
        if q > 1:
            give_back(1, q, True)
    for t in range(2):
        give_back(t, 1, True)

    for q in range(stages):
        for r in range(2):
            origin = source[q] * CORES + (core if r == 0 else 1 - core)
            hot = one_hot(metas[origin][3:4, :], cap)
            part_dots = dots[(q * 2 + r) * cap:(q * 2 + r + 1) * cap, 0:1]
            line = jnp.sum(hot * part_dots, axis=0, keepdims=True)
            route_out[origin] = jnp.broadcast_to(line, (8, count))
    for off in range(1, groups):
        other = (me + off) % groups
        send(None, route_out.at[other], route_in.at[me], route_send.at[off - 1],
             route_recv.at[off - 1], {"expert": other})
    route_in[me] = route_out[me]

    values = weight_slice(dp)
    for h in range(2):
        for i, v in enumerate(pieces(*values, h)):
            own[i, h] = v

    give_back(1, last, False)
    for i in range(3):
        for k, where in ((0, to_y), (1, to_x)):
            landed(grx.at[i, k], gr_recv.at[i, k])
            gs2[i, k] = (keep[i, k] + grx[i, k].astype(F32)).astype(BF16)
            send(None, gs2.at[i, k], grx.at[i, 4 + k], gr_send.at[i, 4 + k], gr_recv.at[i, 4 + k],
                 where)
    for q in near:
        give_back(1, q, False)

    def finish(t, ref):
        for k in range(len(chunks)):
            wait_chunk(has_up, chip + 1 == stages - 1, k, ret_in.at[t, chip], ret_recv.at[t, chip, k])
            wait_chunk(has_down, chip - 1 == 0, k, ret_down.at[t], retd_recv.at[t, k])
        value = ex[...] + tn(up_hot, ret_in[t, chip]) + tn(down_hot, ret_down[t])
        ref[...] = value.astype(BF16)

    def stay(t):
        landed(yy.at[t, 0, pl.ds(cap, cap)], pc_recv.at[t, 0])
        ex[...] = expand(t, 0, 3, 4)

    stay(0)
    finish(0, out_ref)
    stay(1)
    for off in range(1, groups):
        copy(route_out.at[0], route_in.at[0], route_send.at[off - 1], route_recv.at[off - 1],
             to_mate).wait_recv()
    for k, hit in enumerate(hits):
        line = sum(hit[e:e + 1] * route_in[e, 0:1] for e in range(groups))
        route_ref[k:k + 1, :] = line
    for i in range(3):
        for h in range(2):
            landed(grx.at[i, 2 + h], gr_recv.at[i, 2 + h])
            own[i, h] = own[i, h] + grx[i, 2 + h].astype(F32)
    finish(1, tgrad_ref)
    for i, ref in enumerate((gg_ref, ug_ref, dg_ref)):
        for h in range(2):
            landed(grx.at[i, 4 + h], gr_recv.at[i, 4 + h])
            ref[halves[h]] = (own[i, h] + grx[i, 4 + h].astype(F32)).astype(BF16)
    for cond, args in pending:
        if cond is None:
            copy(*args).wait_send()
        else:
            pl.when(cond)(lambda args=args: copy(*args).wait_send())


def flush_kernel(*refs):
    number = (len(refs) - 1) // 2
    copies = [
        pltpu.make_async_copy(refs[n], refs[number + n], refs[-1].at[n]) for n in range(number)
    ]
    for cp in copies:
        cp.start()
    for cp in copies:
        cp.wait()


def flush(*arrays):
    return pl.pallas_call(
        flush_kernel,
        out_shape=tuple(jax.ShapeDtypeStruct(a.shape, a.dtype) for a in arrays),
        in_specs=[pl.BlockSpec(memory_space=pltpu.VMEM)] * len(arrays),
        out_specs=(pl.BlockSpec(memory_space=pltpu.HBM),) * len(arrays),
        scratch_shapes=[pltpu.SemaphoreType.DMA((len(arrays),))],
    )(*(pltpu.with_memory_space_constraint(a, pltpu.VMEM) for a in arrays))


def kernel_scratch(groups, ndp, cap, count, width, part, ff):
    stages = groups // CORES
    rows = groups * cap
    hp = part // 2
    shapes = [
        ((count, width), BF16),
        ((count, width), BF16),
        ((groups, 8, count), F32),
        ((2, 2, stages, count, width), BF16),
        ((2, count, width), BF16),
        ((groups, 8, count), F32),
        ((rows, width), BF16),
        ((rows, width), BF16),
        ((rows, 128), F32),
        ((ndp, part, 2 * ff), BF16),
        ((ndp, part, ff), BF16),
        ((2, stages, 2 * cap, width), BF16),
        ((2, stages, cap, width), BF16),
        ((2, stages, count, width), BF16),
        ((2, count, width), BF16),
        ((2, stages, count, width), BF16),
        ((rows, ff), F32),
        ((rows, ff), F32),
        ((rows, ff), BF16),
        ((rows, ff), BF16),
        ((rows, 2 * ff), BF16),
        ((rows, 128), F32),
        ((3, 4, hp, ff), BF16),
        ((3, 2, hp, ff), BF16),
        ((3, 6, hp, ff), BF16),
        ((3, 2, hp, ff), F32),
        ((3, 2, hp, ff), F32),
        ((count, width), F32),
        ((groups, 8, count), F32),
        ((groups, 8, count), F32),
    ]
    sems = [
        (2, stages, 3, 2), (2, 2, stages, 2), (groups - 1,), (groups - 1,), (3, 6), (3, 6),
        (2, stages), (2, stages), (2, stages, 4), (2, stages, 4), (2, 4), (groups - 1,),
        (groups - 1,), (3, 6), (3, 6), (5,),
    ]
    return shapes, sems


def scratch_bytes(shapes):
    total = 0
    for shape, dtype in shapes:
        size = jnp.dtype(dtype).itemsize
        for n in shape:
            size *= n
        total += size
    return total


def slot_capacity(count, top, experts):
    return max(2, (3 * count * top + 2 * experts - 1) // (2 * experts))


def line_body(groups, ndp, tokens, expert_ids, route_weights, w_gate, w_up, w_down, grad_out):
    count, width = tokens.shape
    _, part, ff = w_gate.shape
    top = expert_ids.shape[1]
    slots = slot_capacity(count, top, groups)
    cap = pad16(slots)
    edge = min(count, pad16(CORES * slots))
    shapes, sems = kernel_scratch(groups, ndp, cap, count, width, part, ff)
    vmem = pl.BlockSpec(memory_space=pltpu.VMEM)
    hbm = pl.BlockSpec(memory_space=pltpu.HBM)
    outs = pl.pallas_call(
        functools.partial(moe_kernel, groups, ndp, cap, edge),
        out_shape=(
            pltpu.VMEM((count, width), BF16),
            pltpu.VMEM((count, width), BF16),
            pltpu.VMEM((top, count), F32),
            pltpu.VMEM((part, ff), BF16),
            pltpu.VMEM((part, ff), BF16),
            pltpu.VMEM((part, ff), BF16),
        ),
        in_specs=[hbm, hbm, vmem, vmem, hbm, hbm, hbm],
        out_specs=(vmem,) * 6,
        scratch_shapes=[pltpu.VMEM(s, d) for s, d in shapes]
        + [pltpu.SemaphoreType.DMA(s) for s in sems],
        compiler_params=pltpu.CompilerParams(
            collective_id=0, has_side_effects=True, vmem_limit_bytes=VMEM_MAX
        ),
    )(tokens, grad_out, expert_ids.T, route_weights.T, w_gate[0], w_up[0], w_down[0])
    layer_out, token_grad, route, gate_g, up_g, down_g = flush(*outs)
    return layer_out, token_grad, route.T, gate_g[None], up_g[None], down_g[None]


def pick_body(groups, ndp, *args):
    tokens, expert_ids, _, w_gate = args[:4]
    count, width = tokens.shape
    local, part, ff = w_gate.shape
    if local == 1 and groups == 4 * CORES and ndp == 4:
        slots = slot_capacity(count, expert_ids.shape[1], groups)
        shapes, _ = kernel_scratch(groups, ndp, pad16(slots), count, width, part, ff)
        tiled = count % 32 == 0 and part % 128 == 0 and ff % 128 == 0
        tiled = tiled and 4 * slots > count and pad16(CORES * slots) < count
        if tiled and scratch_bytes(shapes) < VMEM_MAX * 9 // 10:
            return line_body(groups, ndp, *args)
    return body(*args)


def solution(mesh):
    in_specs = (
        P(("dp", "expert"), None),
        P(("dp", "expert"), None),
        P(("dp", "expert"), None),
        P("expert", "dp", None),
        P("expert", "dp", None),
        P("expert", "dp", None),
        P(("dp", "expert"), None),
    )
    out_specs = (
        P(("dp", "expert"), None),
        P(("dp", "expert"), None),
        P(("dp", "expert"), None),
        P("expert", "dp", None),
        P("expert", "dp", None),
        P("expert", "dp", None),
    )
    step = functools.partial(pick_body, mesh.shape["expert"], mesh.shape["dp"])
    return jax.shard_map(step, mesh=mesh, in_specs=in_specs, out_specs=out_specs, check_vma=False)
```

```python
import functools

import jax
import jax.numpy as jnp
from jax import lax
from jax.experimental import pallas as pl
from jax.experimental.pallas import tpu as pltpu
from jax.sharding import PartitionSpec as P

BF16 = jnp.bfloat16
F32 = jnp.float32
CORES = 2
VMEM_MAX = 56 * 1024 * 1024


def slot_table(expert_ids, experts, capacity):
    flat = expert_ids.reshape(-1)
    count = flat.shape[0]
    same = flat[:, None] == flat[None, :]
    earlier = lax.broadcasted_iota(jnp.int32, (count, count), 0) > lax.broadcasted_iota(
        jnp.int32, (count, count), 1
    )
    rank = jnp.sum((same & earlier).astype(jnp.int32), axis=1)
    target = flat * capacity + rank
    columns = lax.broadcasted_iota(jnp.int32, (count, experts * capacity), 1)
    return (target[:, None] == columns).astype(jnp.bfloat16)


def contract_last(left, right):
    return lax.dot_general(
        left, right, (((1,), (1,)), ((), ())), preferred_element_type=jnp.float32
    )


def contract_first(left, right):
    return lax.dot_general(
        left, right, (((0,), (0,)), ((), ())), preferred_element_type=jnp.float32
    )


def expert_forward(rows, gate_w, up_w, down_w):
    gate = jnp.dot(rows, gate_w, preferred_element_type=jnp.float32)
    up = jnp.dot(rows, up_w, preferred_element_type=jnp.float32)
    sig = jax.nn.sigmoid(gate)
    hidden = (gate * sig * up).astype(jnp.bfloat16)
    expert_out = contract_last(hidden, down_w).astype(jnp.bfloat16)
    return (expert_out, (gate, up, sig, hidden))


def expert_backward(out_grad, saved, gate_w, up_w, down_w):
    gate, up, sig, hidden = saved
    hidden_grad = jnp.dot(out_grad, down_w, preferred_element_type=jnp.float32)
    gate_term = (hidden_grad * up * sig * (1.0 + gate * (1.0 - sig))).astype(jnp.bfloat16)
    up_term = (hidden_grad * gate * sig).astype(jnp.bfloat16)
    slot_grad = (contract_last(gate_term, gate_w) + contract_last(up_term, up_w)).astype(
        jnp.bfloat16
    )
    return (slot_grad, gate_term, up_term)


def weight_grads(rows, out_grad, gate_term, up_term, hidden):
    part_rows, part_grad = (
        lax.all_to_all(rows, "dp", split_axis=1, concat_axis=0, tiled=True),
        lax.all_to_all(out_grad, "dp", split_axis=1, concat_axis=0, tiled=True),
    )
    all_gate, all_up, all_hidden = (
        lax.all_gather(gate_term, "dp", axis=0, tiled=True),
        lax.all_gather(up_term, "dp", axis=0, tiled=True),
        lax.all_gather(hidden, "dp", axis=0, tiled=True),
    )
    down_g = contract_first(part_grad, all_hidden).astype(jnp.bfloat16)
    gate_g = contract_first(part_rows, all_gate).astype(jnp.bfloat16)
    up_g = contract_first(part_rows, all_up).astype(jnp.bfloat16)
    return (gate_g, up_g, down_g)


def body(tokens, expert_ids, route_weights, w_gate, w_up, w_down, grad_out):
    local = w_gate.shape[0]
    groups = lax.axis_size("expert")
    experts = local * groups
    count = tokens.shape[0]
    top = expert_ids.shape[1]
    width = tokens.shape[1]
    capacity = max(2, (3 * count * top + 2 * experts - 1) // (2 * experts))
    table = slot_table(expert_ids, experts, capacity)
    per_token = jnp.sum(table.reshape(count, top, experts * capacity), axis=1)
    send_rows = jnp.dot(per_token.T, tokens, preferred_element_type=jnp.float32)
    send_rows = send_rows.astype(jnp.bfloat16).reshape(experts, capacity, width)
    weighted = (route_weights[:, :, None] * grad_out.astype(jnp.float32)[:, None, :]).astype(
        jnp.bfloat16
    )
    send_grad = jnp.dot(
        table.T, weighted.reshape(count * top, width), preferred_element_type=jnp.float32
    )
    send_grad = send_grad.astype(jnp.bfloat16).reshape(experts, capacity, width)
    full_gate, full_up, full_down = (
        lax.all_gather(w_gate, "dp", axis=1, tiled=True),
        lax.all_gather(w_up, "dp", axis=1, tiled=True),
        lax.all_gather(w_down, "dp", axis=1, tiled=True),
    )
    received = lax.all_to_all(send_rows, "expert", split_axis=0, concat_axis=0, tiled=True)
    shaped = received.reshape(groups, local, capacity, width)
    saves = []
    inputs = []
    slot_expert = 0
    rows = shaped[:, slot_expert].reshape(groups * capacity, width)
    expert_out, saved = expert_forward(
        rows, full_gate[slot_expert], full_up[slot_expert], full_down[slot_expert]
    )
    outs = expert_out.reshape(groups, 1, capacity, width)
    saves.append(saved)
    inputs.append(rows)
    expert_outs, saves, inputs = (outs.reshape(experts, capacity, width), saves, inputs)
    back_out = lax.all_to_all(expert_outs, "expert", split_axis=0, concat_axis=0, tiled=True)
    received_grad = lax.all_to_all(send_grad, "expert", split_axis=0, concat_axis=0, tiled=True)
    shaped = received_grad.reshape(groups, local, capacity, width)
    slot_expert = 0
    out_grad = shaped[:, slot_expert].reshape(groups * capacity, width)
    slot_grad, gate_term, up_term = expert_backward(
        out_grad,
        saves[slot_expert],
        full_gate[slot_expert],
        full_up[slot_expert],
        full_down[slot_expert],
    )
    grads_in = slot_grad.reshape(groups, 1, capacity, width)
    gate_g, up_g, down_g = weight_grads(
        inputs[slot_expert], out_grad, gate_term, up_term, saves[slot_expert][3]
    )
    gate_list = [gate_g]
    up_list = [up_g]
    down_list = [down_g]
    slot_grads = grads_in.reshape(experts, capacity, width)
    gate_grad = jnp.stack(gate_list)
    up_grad = jnp.stack(up_list)
    down_grad = jnp.stack(down_list)
    back_grad = lax.all_to_all(slot_grads, "expert", split_axis=0, concat_axis=0, tiled=True)
    out_slots = jnp.dot(
        table, back_out.reshape(experts * capacity, width), preferred_element_type=jnp.float32
    )
    out_slots = out_slots.reshape(count, top, width)
    layer_out = jnp.sum(route_weights[:, :, None] * out_slots, axis=1).astype(jnp.bfloat16)
    route_grad = jnp.sum(grad_out.astype(jnp.float32)[:, None, :] * out_slots, axis=2)
    grad_slots = jnp.dot(
        table, back_grad.reshape(experts * capacity, width), preferred_element_type=jnp.float32
    )
    token_grad = jnp.sum(grad_slots.reshape(count, top, width), axis=1).astype(jnp.bfloat16)
    return (layer_out, token_grad, route_grad, gate_grad, up_grad, down_grad)


def pad16(n):
    return (n + 15) // 16 * 16


def route_tables(ids, weights, groups, chip):
    top, count = ids.shape
    stages = groups // CORES
    lanes = lax.broadcasted_iota(jnp.int32, (1, count), 1).astype(F32)
    experts = lax.broadcasted_iota(jnp.int32, (groups, count), 0)
    hits = [(ids[k:k + 1, :] == experts).astype(F32) for k in range(top)]
    member = sum(hits)
    weight = sum(hit * weights[k:k + 1, :] for k, hit in enumerate(hits))
    first_up = sum(member[groups - CORES + i:groups - CORES + i + 1] for i in range(CORES))
    first_down = sum(member[i:i + 1] for i in range(CORES))
    first = [(f > 0).astype(F32) for f in (first_up, first_down)]
    before = (
        lax.broadcasted_iota(jnp.int32, (count, count), 0) < lax.broadcasted_iota(jnp.int32, (count, count), 1)
    ).astype(BF16)
    counts = jnp.dot(jnp.concatenate([member] + first + [jnp.zeros((groups - 2, count), F32)], axis=0).astype(BF16),
                     before, preferred_element_type=F32)
    slot = jnp.where(member > 0, counts[:groups], -1.0)

    def position(i):
        ahead = counts[groups + i:groups + i + 1]
        number = jnp.sum(first[i], axis=1, keepdims=True)
        return jnp.where(first[i] > 0, ahead, number + lanes - ahead)

    hots = [one_hot(position(i), count) for i in range(2)]
    def tables():
        dest = lax.broadcasted_iota(jnp.int32, (groups, count), 0) // CORES

        def in_order(values, precision):
            up, down = [
                lax.dot_general(values, hot.astype(values.dtype), (((1,), (1,)), ((), ())),
                                precision=precision, preferred_element_type=F32)
                for hot in hots
            ]
            return jnp.where(dest >= chip, up, down)

        slot_rows = in_order(slot.astype(BF16), None)
        weight_rows = in_order(weight, lax.Precision.HIGHEST)
        tiles = []
        for e in range(groups):
            other = e // CORES * CORES + (CORES - 1 - e % CORES)
            row = lambda a, i: a[i:i + 1]
            tiles.append(jnp.concatenate(
                [row(slot_rows, e), row(weight_rows, e), row(slot_rows, other), row(slot, e), row(slot, other),
                 jnp.zeros((3, count), F32)], axis=0))
        return tiles

    return tables, hots[0].astype(BF16), hots[1].astype(BF16), hits


def one_hot(row, height):
    rows = lax.broadcasted_iota(jnp.int32, (height, row.shape[1]), 0).astype(F32)
    return (rows == row).astype(F32)


def choose(index, values):
    result = jnp.int32(values[0])
    for i in range(1, len(values)):
        result = jnp.where(index == i, jnp.int32(values[i]), result)
    return result


def visit_order(chip, stages):
    inner = -1 if 2 * chip >= stages else 1
    near = [s for d in range(stages) for s in ((chip + d * inner, chip - d * inner) if d else (chip,))]
    return [s for s in near if 0 <= s < stages]


def moe_kernel(
    groups, ndp, cap, edge,
    tok_hbm, grad_hbm, ids_ref, weight_ref, wg_hbm, wu_hbm, wd_hbm,
    out_ref, tgrad_ref, route_ref, gg_ref, ug_ref, dg_ref,
    tok, grad, meta_own, blocks, own_down, metas, xr, gr, wr, wgu, wd, yy, ym, ret_in, ret_down, ret_out,
    fa, fb, hid, hs, both, dots, gs, gs2, grx, keep, own, ex, route_out, route_in,
    in_send, in_recv, meta_send, meta_recv, w_send, w_recv, pc_send, pc_recv,
    ret_send, ret_recv, retd_recv, route_send, route_recv, gr_send, gr_recv, load_sem,
):
    stages = groups // CORES
    count, width = tok.shape
    part, ff = gg_ref.shape
    half, hp = count // 2, part // 2
    me = lax.axis_index("expert")
    dp = lax.axis_index("dp")
    chip, core = me // CORES, me % CORES
    mate = chip * CORES + (1 - core)
    px, py = dp % 2, dp // 2
    xn, yn, dg = py * 2 + (1 - px), (1 - py) * 2 + px, (1 - py) * 2 + (1 - px)
    to_mate, to_x, to_y = {"expert": mate}, {"dp": xn}, {"dp": yn}
    at_edge = (chip == 0) | (chip == stages - 1)
    inside = jnp.logical_not(at_edge)
    has_up, has_down = chip < stages - 1, chip > 0
    up_dev, down_dev = {"expert": me + CORES}, {"expert": me - CORES}
    low = 2 * chip < stages
    yes = chip >= 0
    pending = []

    def copy(src, dst, ssem, rsem, where):
        return pltpu.make_async_remote_copy(
            src_ref=src, dst_ref=dst, send_sem=ssem, recv_sem=rsem,
            device_id=where, device_id_type=pl.DeviceIdType.MESH,
        )

    def send(cond, *args):
        if cond is None:
            copy(*args).start()
        else:
            pl.when(cond)(lambda: copy(*args).start())
        pending.append((cond, args))

    def landed(ref, sem):
        copy(ref, ref, sem, sem, to_mate).wait_recv()

    def rows_of(c, short):
        end = half if c == 0 else (edge if short else count)
        return pl.ds(c * half, end - c * half)

    def send_rows(cond, short, c, src, dst, ssem, rsem, where):
        if c == 0 or edge == count:
            send(cond, src.at[rows_of(c, False)], dst.at[rows_of(c, False)], ssem, rsem, where)
            return
        full = jnp.logical_not(short)
        if cond is not None:
            short, full = cond & short, cond & full
        for when, cut in ((full, rows_of(c, False)), (short, rows_of(c, True))):
            send(when, src.at[cut], dst.at[cut], ssem, rsem, where)

    def wait_rows(cond, short, c, dst, sem):
        if c == 0 or edge == count:
            pl.when(cond)(lambda: landed(dst.at[rows_of(c, False)], sem))
            return
        pl.when(cond & jnp.logical_not(short))(lambda: landed(dst.at[rows_of(c, False)], sem))
        pl.when(cond & short)(lambda: landed(dst.at[rows_of(c, True)], sem))

    def nt(a, b):
        return lax.dot_general(a, b, (((1,), (1,)), ((), ())), preferred_element_type=F32)

    def tn(a, b):
        return lax.dot_general(a, b, (((0,), (0,)), ((), ())), preferred_element_type=F32)

    def nn(a, b):
        return jnp.dot(a, b, preferred_element_type=F32)

    gate_cols, up_cols = pl.ds(0, ff), pl.ds(ff, ff)

    def weight(i, j):
        return wd.at[j] if i == 2 else wgu.at[j, :, gate_cols if i == 0 else up_cols]

    loads = [
        pltpu.make_async_copy(src, dst, load_sem.at[n])
        for n, (src, dst) in enumerate((
            (tok_hbm, tok), (wg_hbm, weight(0, dp)), (wu_hbm, weight(1, dp)), (grad_hbm, grad),
            (wd_hbm, weight(2, dp)),
        ))
    ]
    for load in loads:
        load.start()

    barrier = pltpu.get_barrier_semaphore()
    for off in range(1, groups):
        pl.semaphore_signal(barrier, inc=1, device_id={"expert": (me + off) % groups},
                            device_id_type=pl.DeviceIdType.MESH)
    for off in range(1, ndp):
        pl.semaphore_signal(barrier, inc=1, device_id={"dp": (dp + off) % ndp},
                            device_id_type=pl.DeviceIdType.MESH)

    tables, up_hot, down_hot, hits = route_tables(ids_ref[...], weight_ref[...], groups, chip)

    def arrange(t):
        value = (tok, grad)[t][...]
        blocks[0, t, chip] = nn(up_hot, value).astype(BF16)
        own_down[t] = nn(down_hot, value).astype(BF16)

    loads[0].wait()
    arrange(0)
    pl.semaphore_wait(barrier, groups + ndp - 2)

    def depart_up(t, cond, chunks=(0, 1)):
        for c in chunks:
            send_rows(cond, chip + 1 == stages - 1, c, blocks.at[0, t, chip], blocks.at[0, t, chip],
                      in_send.at[t, 0, 0, c], in_recv.at[0, t, chip, c], up_dev)

    def depart_down(t, cond, chunks=(0, 1)):
        for c in chunks:
            send_rows(cond, chip - 1 == 0, c, own_down.at[t], blocks.at[0, t, chip],
                      in_send.at[t, 0, 1, c], in_recv.at[0, t, chip, c], down_dev)

    def depart_mate(t):
        send(None, blocks.at[0, t, chip], blocks.at[1, t, chip],
             in_send.at[t, 0, 2, 0], in_recv.at[1, t, chip, 0], to_mate)

    halves = (pl.ds(0, hp), pl.ds(hp, hp))

    def weight_direct(i):
        for n, (h, where) in enumerate(((0, to_x), (1, to_y), (1, to_x), (0, to_y))):
            ref = weight(i, dp).at[halves[h]]
            send(None, ref, ref, w_send.at[i, n], w_recv.at[i, n], where)

    def weight_relay(i):
        for n, (h, j, where) in enumerate(((0, xn, to_y), (1, yn, to_x))):
            ref = weight(i, j).at[halves[h]]
            landed(ref, w_recv.at[i, n])
            send(None, ref, ref, w_send.at[i, 4 + n], w_recv.at[i, 4 + n], where)

    def weight_rest(i, ns=range(2, 6)):
        for n in ns:
            h, j = ((1, xn), (0, yn), (0, dg), (1, dg))[n - 2]
            landed(weight(i, j).at[halves[h]], w_recv.at[i, n])

    depart_up(0, has_up)
    depart_down(0, has_down)
    depart_mate(0)
    for i in range(2):
        loads[1 + i].wait()
        weight_direct(i)
    for e, tile in enumerate(tables()):
        meta_own[e] = tile
    for off in range(1, groups):
        other = (me + off) % groups
        send(None, meta_own.at[other], metas.at[me], meta_send.at[off - 1], meta_recv.at[off - 1],
             {"expert": other})
    metas[me] = meta_own[me]
    if edge < count:
        rest = pl.ds(edge, count - edge)
        empty = jnp.zeros((count - edge, width), BF16)
        for s in range(stages):
            ends_at = jnp.where(s > chip, chip - 1, chip + 1)
            from_edge = (s != chip) & inside & ((ends_at == 0) | (ends_at == stages - 1))

            @pl.when(at_edge & (s != chip))
            def _():
                for t in range(2):
                    blocks[0, t, s, rest] = empty
                    blocks[1, t, s, rest] = empty

            @pl.when(from_edge | ((s == chip) & (chip + 1 == stages - 1)))
            def _():
                for t in range(2):
                    ret_in[t, s, rest] = empty

        @pl.when(chip - 1 == 0)
        def _():
            for t in range(2):
                ret_down[t, rest] = empty
    for t in range(2):
        @pl.when(chip == stages - 1)
        def _():
            ret_in[t, chip] = jnp.zeros((count, width), BF16)

        @pl.when(chip == 0)
        def _():
            ret_down[t] = jnp.zeros((count, width), BF16)

    loads[3].wait()
    arrange(1)
    depart_up(1, has_up & at_edge)
    depart_down(1, has_down & at_edge)
    depart_mate(1)
    for off in range(1, groups):
        copy(meta_own.at[0], metas.at[0], meta_send.at[off - 1], meta_recv.at[off - 1],
             to_mate).wait_recv()

    table = [visit_order(z, stages) for z in range(stages)]
    source = [choose(chip, [table[z][q] for z in range(stages)]) for q in range(stages)]

    def arrive(t, q, c, role=yes):
        s = source[q]
        nxt = jnp.where(s < chip, chip + 1, chip - 1)
        more = (nxt >= 0) & (nxt < stages)
        wait_rows(role, at_edge, c, blocks.at[0, t, s], in_recv.at[0, t, s, c])
        send_rows(more & role, (nxt == 0) | (nxt == stages - 1), c, blocks.at[0, t, s],
                  blocks.at[0, t, s], in_send.at[t, q, 0, c], in_recv.at[0, t, s, c],
                  {"expert": nxt * CORES + core})
        send_rows(role, at_edge, c, blocks.at[0, t, s], blocks.at[1, t, s],
                  in_send.at[t, q, 2, c], in_recv.at[1, t, s, c], to_mate)

    def compact(t, q):
        s = source[q]
        for r in range(2):
            if r == 1 and q == 0:
                landed(blocks.at[1, t, s], in_recv.at[1, t, s, 0])
            elif r == 1:
                for c in range(2):
                    wait_rows(yes, at_edge, c, blocks.at[1, t, s], in_recv.at[1, t, s, c])
            tile = metas[s * CORES + (core if r == 0 else 1 - core)]
            hot = one_hot(tile[0:1, :], cap)
            rows = pl.ds((q * 2 + r) * cap, cap)
            (xr, gr)[t][rows, :] = nn(hot.astype(BF16), blocks[r, t, s]).astype(BF16)
            if t == 0:
                scale = jnp.sum(hot * tile[1:2, :], axis=1, keepdims=True)
                wr[rows, :] = jnp.broadcast_to(scale, (cap, 128))

    compact(0, 0)
    near = range(1, stages - 1)
    last = stages - 1
    for q in near:
        arrive(0, q, 0)
    for i in range(2):
        weight_relay(i)
    loads[4].wait()
    weight_direct(2)
    for q in near:
        arrive(0, q, 1)
    for q in near:
        compact(0, q)
    high = jnp.logical_not(low)
    depart_up(1, inside & high, (1,))
    depart_down(1, inside & low, (1,))
    arrive(0, last, 0)
    depart_up(1, inside & low)
    depart_down(1, inside & high)
    arrive(0, last, 1)
    depart_up(1, inside & high, (0,))
    depart_down(1, inside & low, (0,))
    compact(0, last)
    for i in range(2):
        weight_rest(i)

    def cut(j):
        return pl.ds(j * part, part)

    def cut_at(j):
        return pl.ds(pl.multiple_of(j * part, part), part)

    total = xr.shape[0]
    gu = jnp.zeros((total, 2 * ff), F32)
    for j in range(ndp):
        gu += nn(xr[:, cut(j)], wgu[j])
    gate, up = gu[:, :ff], gu[:, ff:]
    sig = jax.nn.sigmoid(gate)
    scale = wr[:, 0:1]
    gated = gate * sig
    value = gated * up
    hid[...] = value.astype(BF16)
    hs[...] = (scale * value).astype(BF16)
    fa[...] = scale * (up * sig * (1.0 + gate * (1.0 - sig)))
    fb[...] = scale * gated

    weight_relay(2)
    arrive(1, 1, 0)
    for q in near[1:]:
        arrive(1, q, 0, inside)
    arrive(1, 1, 1)
    for q in near[1:]:
        arrive(1, q, 1, inside)

    def place(t, cols, value, qs):
        for n, q in enumerate(qs):
            yy[t, q, 0:cap, cols] = value[2 * n * cap:(2 * n + 1) * cap]
            ym[t, q, :, cols] = value[(2 * n + 1) * cap:(2 * n + 2) * cap]

    def pair(t, qs):
        for q in reversed(qs):
            send(None, ym.at[t, q], yy.at[t, q, pl.ds(cap, cap)], pc_send.at[t, q],
                 pc_recv.at[t, q], to_mate)

    everyone = range(stages)
    for n, j in enumerate((dp, xn, yn, dg)):
        if n == 1:
            weight_rest(2, (2, 3))
        if n == 3:
            weight_rest(2, (4, 5))
        place(0, cut_at(j), nt(hs[...], wd[j]).astype(BF16), everyone)
    pair(0, everyone)

    def expand(t, q, row_own, row_mate):
        tile = metas[source[q] * CORES + core]
        hot = jnp.concatenate(
            [one_hot(tile[row_own:row_own + 1, :], cap), one_hot(tile[row_mate:row_mate + 1, :], cap)],
            axis=0).astype(BF16)
        return tn(hot, yy[t, q])

    bounds = (0, half // 2, half, edge, count)
    chunks = [pl.ds(lo, hi - lo) for lo, hi in zip(bounds, bounds[1:])]

    def wait_chunk(cond, short, k, dst, sem):
        if k == len(chunks) - 1:
            cond = cond & jnp.logical_not(short)
        pl.when(cond)(lambda: landed(dst.at[chunks[k]], sem))

    def give_back(t, q, ends):
        s = source[q]
        rising = s > chip
        nxt = jnp.where(rising, chip + 1, chip - 1)
        back = jnp.where(rising, chip - 1, chip + 1)
        where = {"expert": nxt * CORES + core}
        here = at_edge if ends else inside
        arrives = rising & (nxt == s)
        short = (back == 0) | (back == stages - 1)

        @pl.when(here)
        def _():
            landed(yy.at[t, q, pl.ds(cap, cap)], pc_recv.at[t, q])
            ex[...] = expand(t, q, 0, 2)

        for k, rows in enumerate(chunks):
            if ends and k == len(chunks) - 1:
                continue
            if not ends:
                wait_chunk(here, short, k, ret_in.at[t, s], ret_recv.at[t, s, k])

            @pl.when(here)
            def _():
                value = ex[rows]
                if not ends:
                    value = value + ret_in[t, s, rows].astype(F32)
                ret_out[t, q, rows] = value.astype(BF16)

            send(here & arrives, ret_out.at[t, q, rows], ret_down.at[t, rows], ret_send.at[t, q, k],
                 retd_recv.at[t, k], where)
            send(here & jnp.logical_not(arrives), ret_out.at[t, q, rows], ret_in.at[t, s, rows],
                 ret_send.at[t, q, k], ret_recv.at[t, s, k], where)

    def backward_hidden(qs):
        rows = pl.ds(qs[0] * 2 * cap, len(qs) * 2 * cap)
        hg = nn(gr[rows, cut(0)], wd[0])
        for j in range(1, ndp):
            hg += nn(gr[rows, cut(j)], wd[j])
        both[rows, :ff] = (hg * fa[rows, :]).astype(BF16)
        both[rows, ff:] = (hg * fb[rows, :]).astype(BF16)
        line = jnp.sum(hg * hid[rows, :].astype(F32), axis=1, keepdims=True)
        dots[rows, :] = jnp.broadcast_to(line, (line.shape[0], 128))

    def backward_rows(qs):
        rows = pl.ds(qs[0] * 2 * cap, len(qs) * 2 * cap)
        for j in range(ndp):
            place(1, cut(j), nt(both[rows, :], wgu[j]).astype(BF16), qs)
        pair(1, qs)

    give_back(0, last, True)
    for q in reversed(near):
        if q > 1:
            give_back(0, q, True)
    arrive(1, last, 0, inside)
    compact(1, 0)
    compact(1, 1)
    for q in near[1:]:
        for c in range(2):
            arrive(1, q, c, at_edge)
        compact(1, q)
    backward_hidden(range(last))
    backward_rows(range(last))
    arrive(1, last, 1, inside)
    give_back(0, last, False)
    for c in range(2):
        arrive(1, last, c, at_edge)
    compact(1, last)
    backward_hidden(range(last, stages))

    def weight_slice(j):
        cols = cut_at(j)
        return nn_t(xr, cols, both), nn_t(gr, cols, hs)

    def nn_t(rows_ref, cols, ref):
        return tn(rows_ref[:, cols], ref[...])

    def pieces(value, down, h):
        top = slice(h * hp, (h + 1) * hp)
        return value[top, :ff], value[top, ff:], down[top]

    def give_grad(k, h, values, where):
        for i, v in enumerate(pieces(*values, h)):
            gs[i, k] = v.astype(BF16)
        for i in range(3):
            send(None, gs.at[i, k], grx.at[i, k], gr_send.at[i, k], gr_recv.at[i, k], where)

    def keep_grad(k, h, values):
        for i, v in enumerate(pieces(*values, h)):
            keep[i, k] = v

    values = weight_slice(dg)
    give_grad(0, 0, values, to_x)
    give_grad(1, 1, values, to_y)
    backward_rows(range(last, stages))
    values = weight_slice(xn)
    give_grad(2, 0, values, to_x)
    keep_grad(1, 1, values)
    give_back(1, last, True)
    values = weight_slice(yn)
    give_grad(3, 1, values, to_y)
    keep_grad(0, 0, values)
    for q in near:
        give_back(0, q, False)
    for q in reversed(near):
        if q > 1:
            give_back(1, q, True)
    for t in range(2):
        give_back(t, 1, True)

    for q in range(stages):
        for r in range(2):
            origin = source[q] * CORES + (core if r == 0 else 1 - core)
            hot = one_hot(metas[origin][3:4, :], cap)
            part_dots = dots[(q * 2 + r) * cap:(q * 2 + r + 1) * cap, 0:1]
            line = jnp.sum(hot * part_dots, axis=0, keepdims=True)
            route_out[origin] = jnp.broadcast_to(line, (8, count))
    for off in range(1, groups):
        other = (me + off) % groups
        send(None, route_out.at[other], route_in.at[me], route_send.at[off - 1],
             route_recv.at[off - 1], {"expert": other})
    route_in[me] = route_out[me]

    values = weight_slice(dp)
    for h in range(2):
        for i, v in enumerate(pieces(*values, h)):
            own[i, h] = v

    give_back(1, last, False)
    for i in range(3):
        for k, where in ((0, to_y), (1, to_x)):
            landed(grx.at[i, k], gr_recv.at[i, k])
            gs2[i, k] = (keep[i, k] + grx[i, k].astype(F32)).astype(BF16)
            send(None, gs2.at[i, k], grx.at[i, 4 + k], gr_send.at[i, 4 + k], gr_recv.at[i, 4 + k],
                 where)
    for q in near:
        give_back(1, q, False)

    def finish(t, ref):
        for k in range(len(chunks)):
            wait_chunk(has_up, chip + 1 == stages - 1, k, ret_in.at[t, chip], ret_recv.at[t, chip, k])
            wait_chunk(has_down, chip - 1 == 0, k, ret_down.at[t], retd_recv.at[t, k])
        value = ex[...] + tn(up_hot, ret_in[t, chip]) + tn(down_hot, ret_down[t])
        ref[...] = value.astype(BF16)

    def stay(t):
        landed(yy.at[t, 0, pl.ds(cap, cap)], pc_recv.at[t, 0])
        ex[...] = expand(t, 0, 3, 4)

    stay(0)
    finish(0, out_ref)
    stay(1)
    for off in range(1, groups):
        copy(route_out.at[0], route_in.at[0], route_send.at[off - 1], route_recv.at[off - 1],
             to_mate).wait_recv()
    for k, hit in enumerate(hits):
        line = sum(hit[e:e + 1] * route_in[e, 0:1] for e in range(groups))
        route_ref[k:k + 1, :] = line
    for i in range(3):
        for h in range(2):
            landed(grx.at[i, 2 + h], gr_recv.at[i, 2 + h])
            own[i, h] = own[i, h] + grx[i, 2 + h].astype(F32)

    def finish_weights():
        for i, ref in enumerate((gg_ref, ug_ref, dg_ref)):
            for h in range(2):
                landed(grx.at[i, 4 + h], gr_recv.at[i, 4 + h])
                ref[halves[h]] = (own[i, h] + grx[i, 4 + h].astype(F32)).astype(BF16)

    pl.when(inside)(finish_weights)
    finish(1, tgrad_ref)
    pl.when(at_edge)(finish_weights)
    for cond, args in pending:
        if cond is None:
            copy(*args).wait_send()
        else:
            pl.when(cond)(lambda args=args: copy(*args).wait_send())


def flush_kernel(*refs):
    number = (len(refs) - 1) // 2
    copies = [
        pltpu.make_async_copy(refs[n], refs[number + n], refs[-1].at[n]) for n in range(number)
    ]
    for cp in copies:
        cp.start()
    for cp in copies:
        cp.wait()


def flush(*arrays):
    return pl.pallas_call(
        flush_kernel,
        out_shape=tuple(jax.ShapeDtypeStruct(a.shape, a.dtype) for a in arrays),
        in_specs=[pl.BlockSpec(memory_space=pltpu.VMEM)] * len(arrays),
        out_specs=(pl.BlockSpec(memory_space=pltpu.HBM),) * len(arrays),
        scratch_shapes=[pltpu.SemaphoreType.DMA((len(arrays),))],
    )(*(pltpu.with_memory_space_constraint(a, pltpu.VMEM) for a in arrays))


def kernel_scratch(groups, ndp, cap, count, width, part, ff):
    stages = groups // CORES
    rows = groups * cap
    hp = part // 2
    shapes = [
        ((count, width), BF16),
        ((count, width), BF16),
        ((groups, 8, count), F32),
        ((2, 2, stages, count, width), BF16),
        ((2, count, width), BF16),
        ((groups, 8, count), F32),
        ((rows, width), BF16),
        ((rows, width), BF16),
        ((rows, 128), F32),
        ((ndp, part, 2 * ff), BF16),
        ((ndp, part, ff), BF16),
        ((2, stages, 2 * cap, width), BF16),
        ((2, stages, cap, width), BF16),
        ((2, stages, count, width), BF16),
        ((2, count, width), BF16),
        ((2, stages, count, width), BF16),
        ((rows, ff), F32),
        ((rows, ff), F32),
        ((rows, ff), BF16),
        ((rows, ff), BF16),
        ((rows, 2 * ff), BF16),
        ((rows, 128), F32),
        ((3, 4, hp, ff), BF16),
        ((3, 2, hp, ff), BF16),
        ((3, 6, hp, ff), BF16),
        ((3, 2, hp, ff), F32),
        ((3, 2, hp, ff), F32),
        ((count, width), F32),
        ((groups, 8, count), F32),
        ((groups, 8, count), F32),
    ]
    sems = [
        (2, stages, 3, 2), (2, 2, stages, 2), (groups - 1,), (groups - 1,), (3, 6), (3, 6),
        (2, stages), (2, stages), (2, stages, 4), (2, stages, 4), (2, 4), (groups - 1,),
        (groups - 1,), (3, 6), (3, 6), (5,),
    ]
    return shapes, sems


def scratch_bytes(shapes):
    total = 0
    for shape, dtype in shapes:
        size = jnp.dtype(dtype).itemsize
        for n in shape:
            size *= n
        total += size
    return total


def slot_capacity(count, top, experts):
    return max(2, (3 * count * top + 2 * experts - 1) // (2 * experts))


def line_body(groups, ndp, tokens, expert_ids, route_weights, w_gate, w_up, w_down, grad_out):
    count, width = tokens.shape
    _, part, ff = w_gate.shape
    top = expert_ids.shape[1]
    slots = slot_capacity(count, top, groups)
    cap = pad16(slots)
    edge = min(count, pad16(CORES * slots))
    shapes, sems = kernel_scratch(groups, ndp, cap, count, width, part, ff)
    vmem = pl.BlockSpec(memory_space=pltpu.VMEM)
    hbm = pl.BlockSpec(memory_space=pltpu.HBM)
    outs = pl.pallas_call(
        functools.partial(moe_kernel, groups, ndp, cap, edge),
        out_shape=(
            pltpu.VMEM((count, width), BF16),
            pltpu.VMEM((count, width), BF16),
            pltpu.VMEM((top, count), F32),
            pltpu.VMEM((part, ff), BF16),
            pltpu.VMEM((part, ff), BF16),
            pltpu.VMEM((part, ff), BF16),
        ),
        in_specs=[hbm, hbm, vmem, vmem, hbm, hbm, hbm],
        out_specs=(vmem,) * 6,
        scratch_shapes=[pltpu.VMEM(s, d) for s, d in shapes]
        + [pltpu.SemaphoreType.DMA(s) for s in sems],
        compiler_params=pltpu.CompilerParams(
            collective_id=0, has_side_effects=True, vmem_limit_bytes=VMEM_MAX
        ),
    )(tokens, grad_out, expert_ids.T, route_weights.T, w_gate[0], w_up[0], w_down[0])
    layer_out, token_grad, route, gate_g, up_g, down_g = flush(*outs)
    return layer_out, token_grad, route.T, gate_g[None], up_g[None], down_g[None]


def pick_body(groups, ndp, *args):
    tokens, expert_ids, _, w_gate = args[:4]
    count, width = tokens.shape
    local, part, ff = w_gate.shape
    if local == 1 and groups == 4 * CORES and ndp == 4:
        slots = slot_capacity(count, expert_ids.shape[1], groups)
        shapes, _ = kernel_scratch(groups, ndp, pad16(slots), count, width, part, ff)
        tiled = count % 32 == 0 and part % 128 == 0 and ff % 128 == 0
        tiled = tiled and 4 * slots > count and pad16(CORES * slots) < count
        if tiled and scratch_bytes(shapes) < VMEM_MAX * 9 // 10:
            return line_body(groups, ndp, *args)
    return body(*args)


def solution(mesh):
    in_specs = (
        P(("dp", "expert"), None),
        P(("dp", "expert"), None),
        P(("dp", "expert"), None),
        P("expert", "dp", None),
        P("expert", "dp", None),
        P("expert", "dp", None),
        P(("dp", "expert"), None),
    )
    out_specs = (
        P(("dp", "expert"), None),
        P(("dp", "expert"), None),
        P(("dp", "expert"), None),
        P("expert", "dp", None),
        P("expert", "dp", None),
        P("expert", "dp", None),
    )
    step = functools.partial(pick_body, mesh.shape["expert"], mesh.shape["dp"])
    return jax.shard_map(step, mesh=mesh, in_specs=in_specs, out_specs=out_specs, check_vma=False)
```
